128 devices in a mesh: ma: 32 (over y, z, core), pb: 4 (over x).
Axes of the slice: x: 4, y: 4, z: 4, core: 2. Of those that a mesh axis runs over, the one named last changes fastest.
Arguments:
- coefs: float32 [512, 1056, 64], P('ma', 'pb'), may hold values from -6 to 6
- legendre: float32 [512, 1056, 4, 256], P('ma', None, 'pb'), may hold values from -0.25 to 0.25
- quad_weight: float32 [4, 256], P('pb'), may hold values from 0.3 to 3
- pair_of_slot: int32 [512], replicated, may hold values from 0 to 511, each once
- tracers: float32 [12, 2, 1024, 2048], P(None, None, ('ma', 'pb')), may hold values from 0 to 2
- heat_rate: float32 [12, 2], replicated, may hold values from -1.75 to 1.75
Outputs:
- spec_tendency: float32 [512, 1056, 64], P('ma', 'pb')
- tracers_new: float32 [12, 2, 1024, 2048], P(None, None, ('ma', 'pb'))
The draws below stay inside these ranges and needn't reach their ends.
Inputs may be any that keep to these rules, and one draw needn't show every extreme that they name: Each pair number appears once; slot s holds the orders pair_of_slot[s] and 1023 - pair_of_slot[s].
All inputs are finite; a program needn't handle non-finite values.
Results may differ from the reference program's by a relative error of at most 0.00007.
Values sent between devices are 32-bit elements; how exact they have to be, the bound alone decides.
No kernel may reach another device: no remote copies, remote signals or barrier semaphores. Data moves between devices by JAX's collectives and lax.ppermute only.
A program may use at most 128 MiB of HBM per device.

```python
import math
import jax
import jax.numpy as jnp
from jax import lax

M = 1024
NLAT = 1024
NLON = 2048
LAYER_TOTAL = 8
NF = 4
NTR = 12
TLEV = 2
PAIRS = 512
PROWS = 1056
COLS = 64
QLAT = 256
BAND = 8
N_MA = 32
N_PB = 4


def steps_of(rng, dims, shards, low, largest):
    loudness = 1.0
    for dim, shards_of in shards:
        heights = jax.random.uniform(jax.random.fold_in(jax.random.fold_in(rng, 6), dim), (shards_of,), jnp.float32, low / len(shards), largest / len(shards))
        loudness = loudness * jnp.repeat(jnp.exp(heights), dims[dim] // shards_of).reshape((-1,) + (1,) * (len(dims) - 1 - dim))
    return loudness


def scatter_about(rng, extent, spread, most, shards=(), held_as=jnp.bfloat16):
    array = spread * jax.random.normal(rng, extent, jnp.float32)
    if shards:
        array = array * steps_of(rng, extent, shards, -0.22, 0.18)
    return jnp.clip(array, -most, most).astype(held_as)


def setup_inputs(seed: int = 0) -> dict:
    arg_keys = jax.random.split(jax.random.key(seed), 7)
    return {
        "coefs": scatter_about(arg_keys[0], (PAIRS, PROWS, COLS), 1.0, 6.0, ((0, 32), (1, 4)), jnp.float32),
        "legendre": scatter_about(arg_keys[1], (PAIRS, PROWS, N_PB, QLAT), (M // 2) ** -0.5, 0.25, ((0, 32), (2, 4)), jnp.float32),
        "quad_weight": jnp.clip(jnp.exp(math.log(3.0) - 2.3025851 * jax.random.uniform(arg_keys[2], (N_PB, QLAT), jnp.float32) ** steps_of(arg_keys[2], (N_PB, QLAT), ((0, 4),), -0.2, 0.2)), 0.3, 3.0),
        "pair_of_slot": jax.random.permutation(arg_keys[3], PAIRS).astype(jnp.int32),
        "tracers": jnp.clip(2.0 * jax.random.uniform(arg_keys[4], (NTR, TLEV, NLAT, NLON), jnp.float32) ** steps_of(arg_keys[4], (NTR, TLEV, NLAT, NLON), ((2, 128),), -0.2, 0.2), 0.0, 2.0),
        "heat_rate": scatter_about(arg_keys[5], (NTR, TLEV), NTR ** -0.5, 1.75, (), jnp.float32),
    }


COURANT = 0.15
DRAG_COEFFICIENT = 0.2
MOISTURE_SOURCE = 0.3
RAINFALL_FACTOR = 0.2
HIGHEST = lax.Precision.HIGHEST

def order_tables(pair_of_slot):
    lowest = pair_of_slot.astype(jnp.int32)
    orders = jnp.stack([lowest, M - 1 - lowest], axis=1)
    points = jnp.arange(NLON, dtype=jnp.int32)
    phases = orders[:, :, None] * points[None, None, :] % NLON
    angles = phases.astype(jnp.float32) * (2.0 * math.pi / NLON)
    factor = 1.0 / math.sqrt(NLON)
    fourier_table = jnp.stack([jnp.cos(angles) * factor, -jnp.sin(angles) * factor], axis=0)
    weights = jnp.where(orders == 0, 1.0, 2.0).astype(jnp.float32)
    return (fourier_table, weights)

def row_masks(pair_ids, row_start, row_count):
    row_ids = row_start + jnp.arange(row_count, dtype=jnp.int32)
    bounds = (M - pair_ids.astype(jnp.int32))[:, None]
    low_rows = row_ids[None, :] < bounds
    high_rows = (row_ids[None, :] >= bounds) & (row_ids[None, :] <= M)
    return (low_rows, high_rows)

def advect(padded, zonal_wind, southward, first_row):
    middle = padded[:, :, 1:-1, :]
    east_face = 0.5 * (zonal_wind + jnp.roll(zonal_wind, -1, axis=-1))
    flux_east = jnp.maximum(east_face, 0.0) * middle + jnp.minimum(east_face, 0.0) * jnp.roll(middle, -1, axis=-1)
    across = 0.5 * (southward[:, :-1, :] + southward[:, 1:, :])
    flux_south = jnp.maximum(across, 0.0) * padded[:, :, :-1, :] + jnp.minimum(across, 0.0) * padded[:, :, 1:, :]
    upper_row = first_row - 1 + jnp.arange(across.shape[1], dtype=jnp.int32)
    inside = (upper_row >= 0) & (upper_row <= NLAT - 2)
    flux_south = jnp.where(inside[None, None, :, None], flux_south, 0.0)
    change = flux_east - jnp.roll(flux_east, 1, axis=-1) + (flux_south[:, :, 1:, :] - flux_south[:, :, :-1, :])
    return -COURANT * change

def reference(coefs, legendre, quad_weight, pair_of_slot, tracers, heat_rate):
    legendre_rows = legendre.reshape(PAIRS, PROWS, NLAT)
    low_rows, high_rows = row_masks(pair_of_slot, 0, PROWS)
    masked = jnp.concatenate([jnp.where(low_rows[:, :, None], coefs, 0.0), jnp.where(high_rows[:, :, None], coefs, 0.0)], axis=2)
    stored = jnp.einsum('srl,src->slc', legendre_rows, masked, precision=HIGHEST)
    latitudes = stored.reshape(PAIRS, N_PB, N_MA, BAND, 2 * COLS).transpose(0, 2, 1, 3, 4).reshape(PAIRS, NLAT, 2 * COLS)
    fourier_table, weights = order_tables(pair_of_slot)
    spectral = latitudes.reshape(PAIRS, NLAT, 2, 2, NF * LAYER_TOTAL) * weights[:, None, :, None, None]
    physical_space_field = jnp.einsum('sjhpc,pshi->jci', spectral, fourier_table, precision=HIGHEST)
    zonal_wind = jnp.transpose(physical_space_field[:, 0:TLEV, :], (1, 0, 2))
    southward = -jnp.transpose(physical_space_field[:, LAYER_TOTAL:LAYER_TOTAL + TLEV, :], (1, 0, 2))
    southward_ext = jnp.pad(southward, ((0, 0), (1, 1), (0, 0)))

    def runge_section(tracer_field):
        padded = jnp.pad(tracer_field, ((0, 0), (0, 0), (1, 1), (0, 0)))
        return advect(padded, zonal_wind, southward_ext, 0)
    first_section = tracers + runge_section(tracers)
    second = 0.75 * tracers + 0.25 * (first_section + runge_section(first_section))
    tracers_new = tracers / 3.0 + 2.0 / 3.0 * (second + runge_section(second))
    heating = jnp.einsum('kl,klji->jli', heat_rate, tracers_new, precision=HIGHEST)
    eastward_finished = physical_space_field[:, 0:LAYER_TOTAL]
    northward_velocity = physical_space_field[:, LAYER_TOTAL:2 * LAYER_TOTAL]
    thermal_state = physical_space_field[:, 2 * LAYER_TOTAL:3 * LAYER_TOTAL]
    vapour_mixing_share = physical_space_field[:, 3 * LAYER_TOTAL:4 * LAYER_TOTAL]
    flow_speed_norm = jnp.sqrt(eastward_finished * eastward_finished + northward_velocity * northward_velocity + 1.0)
    warming_finished = jnp.pad(heating, ((0, 0), (0, LAYER_TOTAL - TLEV), (0, 0)))
    rate_of_change_field = jnp.concatenate([-DRAG_COEFFICIENT * flow_speed_norm * eastward_finished, -DRAG_COEFFICIENT * flow_speed_norm * northward_velocity, warming_finished - MOISTURE_SOURCE * thermal_state * vapour_mixing_share, MOISTURE_SOURCE * thermal_state * vapour_mixing_share - RAINFALL_FACTOR * flow_speed_norm * vapour_mixing_share], axis=1)
    fourier = jnp.einsum('jci,pshi->sjhpc', rate_of_change_field, fourier_table, precision=HIGHEST).reshape(PAIRS, NLAT, 2 * COLS)
    stored_back = fourier.reshape(PAIRS, N_MA, N_PB, BAND, 2 * COLS).transpose(0, 2, 1, 3, 4).reshape(PAIRS, NLAT, 2 * COLS)
    weighted = stored_back * quad_weight.reshape(NLAT)[None, :, None]
    row_sums = jnp.einsum('srl,slc->src', legendre_rows, weighted, precision=HIGHEST)
    spec_tendency = jnp.where(low_rows[:, :, None], row_sums[:, :, :COLS], 0.0) + jnp.where(high_rows[:, :, None], row_sums[:, :, COLS:], 0.0)
    return (spec_tendency, tracers_new)
```

```python
import math

import jax
import jax.numpy as jnp
from jax import lax
from jax.experimental import pallas as pl
from jax.experimental.pallas import tpu as pltpu
from jax.sharding import PartitionSpec as P

M = 1024
NLAT = 1024
NLON = 2048
HALF = NLON // 2
NTR = 12
TLEV = 2
SLOTS = 16
ROWS = 264
ALL_ROWS = 1056
QLAT = 256

COURANT = 0.15
DRAG_COEFFICIENT = 0.2
MOISTURE_SOURCE = 0.3
RAINFALL_FACTOR = 0.2

BF16 = jnp.bfloat16
F32 = jnp.float32
VMEM_LIMIT = 56 * 1024 * 1024


def params(**kw):
    return pltpu.CompilerParams(vmem_limit_bytes=VMEM_LIMIT, **kw)


def cost(us):
    return pl.CostEstimate(flops=int(us * 2.5e8), bytes_accessed=1 << 20, transcendentals=0)


def split(x):
    hi = x.astype(BF16)
    return hi, (x - hi.astype(F32)).astype(BF16)


def mm(a, b):
    return lax.dot_general(a, b, (((1,), (0,)), ((), ())), preferred_element_type=F32)


def mm_t(a, b):
    return lax.dot_general(a, b, (((1,), (1,)), ((), ())), preferred_element_type=F32)


def pack_kernel(c_ref, a_ref, b_ref, scr):
    for ch, out in ((0, a_ref), (1, b_ref)):
        for g in range(4):
            for s in range(4):
                for p in range(2):
                    r0 = s * 32 + p * 16
                    c0 = p * 32 + ch * 16
                    scr[r0 : r0 + 16, 0:ROWS] = c_ref[4 * g + s, c0 : c0 + 16, :]
            out[g] = scr[...].T[0:ROWS]


def pack(coefs_t):
    shape = jax.ShapeDtypeStruct((4, ROWS, 128), F32)
    return pl.pallas_call(
        pack_kernel,
        out_shape=(shape, shape),
        scratch_shapes=[pltpu.VMEM((128, 384), F32)],
        compiler_params=params(),
        cost_estimate=cost(3),
        name="pack",
    )(coefs_t)


def legendre_kernel(
    pairs, place, own, right, left, far_a, far_b, hi_hbm, lo_hbm,
    out, rows, cols, leg_hi, leg_lo, sem,
):
    step = pl.program_id(0)
    d = place[0]

    def put(k, value):
        start = pl.multiple_of(((d + k) % 4) * ROWS, 8)
        rows[pl.ds(start, ROWS), :] = value

    put(0, own[0])
    put(3, right[0])
    put(1, left[0])
    put(2, jnp.where(step < 2, far_a[0], far_b[0]))
    cols[...] = rows[...].T
    fetch(step, hi_hbm, lo_hbm, leg_hi, leg_lo, sem)
    sums = []
    for q in range(4):
        n = 4 * step + q
        lo_order = pairs[n]
        odd = lo_order % 2
        x = cols[32 * q : 32 * q + 32, 0:M]
        r = lax.broadcasted_iota(jnp.int32, (1, M), 1)
        low = (r < M - lo_order).astype(jnp.int32)
        weight = jnp.where((low == 1) & (lo_order == 0), 1.0, 2.0)
        in_even = low != odd
        x = x * weight
        lhs = jnp.concatenate([jnp.where(in_even, x, 0.0), jnp.where(in_even, 0.0, x)], axis=0)
        hi, lo = split(lhs)
        both = jnp.concatenate([hi, lo], axis=0)
        last = 2.0 * cols[32 * q : 32 * q + 32, M : M + 128][:, 0:1]
        row = leg_hi[n, M : M + 16, :].astype(F32)[0:1] + leg_lo[n, M : M + 16, :].astype(F32)[0:1]
        outer = last * row
        first = mm(both, leg_hi[n, 0:M, :])
        acc = first[0:64] + first[64:128] + mm(hi, leg_lo[n, 0:M, :])
        sums.append(
            acc
            + jnp.concatenate(
                [jnp.where(odd == 1, outer, 0.0), jnp.where(odd == 1, 0.0, outer)], axis=0
            )
        )
    for p in range(2):
        out[:, p] = jnp.concatenate(sums[2 * p : 2 * p + 2], axis=0).T.reshape(32, 8, 128)


def prepare_kernel(leg, hi_out, lo_out, raw, hi_buf, lo_buf, sem):
    step = pl.program_id(0)

    def load(n):
        return pltpu.make_async_copy(leg.at[n], raw.at[n], sem.at[0, n])

    def store(n):
        return (
            pltpu.make_async_copy(hi_buf.at[n], hi_out.at[n], sem.at[1, n]),
            pltpu.make_async_copy(lo_buf.at[n], lo_out.at[n], sem.at[2, n]),
        )

    @pl.when(step == 0)
    def _():
        for n in range(SLOTS):
            load(n).start()

    load(step).wait()
    for t in range(2):
        hi, lo = split(raw[step, pl.ds(t, ALL_ROWS, stride=2), :])
        hi_buf[step, :, 128 * t : 128 * t + 128] = hi
        lo_buf[step, :, 128 * t : 128 * t + 128] = lo
    for copy in store(step):
        copy.start()

    @pl.when(step == SLOTS - 1)
    def _():
        for n in range(SLOTS):
            for copy in store(n):
                copy.wait()


ANY = pl.BlockSpec(memory_space=pl.ANY)


def prepare(leg):
    shape = jax.ShapeDtypeStruct((SLOTS, ALL_ROWS, QLAT), BF16)
    buffer = pltpu.VMEM((SLOTS, ALL_ROWS, QLAT), BF16)
    return pl.pallas_call(
        prepare_kernel,
        grid=(SLOTS,),
        in_specs=[ANY],
        out_specs=(ANY, ANY),
        out_shape=(shape, shape),
        scratch_shapes=[
            pltpu.VMEM((SLOTS, 2 * ALL_ROWS, 128), F32),
            buffer,
            buffer,
            pltpu.SemaphoreType.DMA((3, SLOTS)),
        ],
        compiler_params=params(dimension_semantics=("arbitrary",)),
        cost_estimate=cost(11),
        name="prepare",
    )(leg)


LEG_SCRATCH = [
    pltpu.VMEM((SLOTS, ALL_ROWS, QLAT), BF16),
    pltpu.VMEM((SLOTS, ALL_ROWS, QLAT), BF16),
    pltpu.SemaphoreType.DMA((2, SLOTS)),
]


def fetch(step, hi_hbm, lo_hbm, leg_hi, leg_lo, sem):
    def loads(group):
        return [
            pltpu.make_async_copy(src.at[4 * group + n], dst.at[4 * group + n], sem.at[i, 4 * group + n])
            for n in range(4)
            for i, (src, dst) in enumerate(((hi_hbm, leg_hi), (lo_hbm, leg_lo)))
        ]

    @pl.when(step == 0)
    def _():
        for copy in loads(0):
            copy.start()

    for copy in loads(step):
        copy.wait()

    @pl.when(step == 0)
    def _():
        for copy in loads(1):
            copy.start()

    @pl.when(step < 2)
    def _():
        for copy in loads(step + 2):
            copy.start()


def legendre_sums(pairs, place, own, right, left, far_a, far_b, leg_hi, leg_lo):
    def group(i, *_):
        return (i, 0, 0)

    block = (1, ROWS, 128)
    return pl.pallas_call(
        legendre_kernel,
        grid_spec=pltpu.PrefetchScalarGridSpec(
            num_scalar_prefetch=2,
            grid=(4,),
            in_specs=[
                pl.BlockSpec(block, group),
                pl.BlockSpec(block, group),
                pl.BlockSpec(block, group),
                pl.BlockSpec(block, lambda i, *_: (jnp.minimum(i, 1), 0, 0)),
                pl.BlockSpec(block, lambda i, *_: (jnp.maximum(i - 2, 0), 0, 0)),
                ANY,
                ANY,
            ],
            out_specs=pl.BlockSpec((32, 2, 8, 128), lambda i, *_: (0, i, 0, 0)),
            scratch_shapes=[pltpu.VMEM((1152, 128), F32), pltpu.VMEM((128, 1152), F32)]
            + LEG_SCRATCH,
        ),
        out_shape=jax.ShapeDtypeStruct((32, 8, 8, 128), F32),
        compiler_params=params(dimension_semantics=("arbitrary",)),
        cost_estimate=cost(10),
        name="legendre_sums",
    )(pairs, place, own, right, left, far_a, far_b, leg_hi, leg_lo)


def cos_sin(phase):
    quadrant = (phase + NLON // 8) // (NLON // 4)
    x = (phase - quadrant * (NLON // 4)).astype(F32) * (2.0 * math.pi / NLON)
    y = x * x
    s = x * (1.0 + y * (-1 / 6 + y * (1 / 120 + y * (-1 / 5040 + y * (1 / 362880)))))
    c = 1.0 + y * (-1 / 2 + y * (1 / 24 + y * (-1 / 720 + y * (1 / 40320 + y * (-1 / 3628800)))))
    swap = quadrant % 2 == 1
    cos = jnp.where(swap, s, c)
    sin = jnp.where(swap, c, s)
    cos = jnp.where((quadrant + 1) % 4 >= 2, -cos, cos)
    return cos, jnp.where(quadrant % 4 >= 2, -sin, sin)


def table_kernel(orders, hi_ref, lo_ref):
    m = orders[0]
    product = m * lax.broadcasted_iota(jnp.int32, (1, 128), 1)
    cb, sb = cos_sin(product % NLON)
    factor = 1.0 / math.sqrt(NLON)
    cb, sb = cb * factor, sb * factor
    ca, sa = cos_sin(product % 16 * 128)
    for a in range(8):
        c1, s1 = ca[:, a : a + 1], sa[:, a : a + 1]
        for part, value in ((0, c1 * cb - s1 * sb), (1, -(s1 * cb + c1 * sb))):
            hi, lo = split(value)
            hi_ref[part, :, 128 * a : 128 * a + 128] = hi
            lo_ref[part, :, 128 * a : 128 * a + 128] = lo


def fourier_tables(pair_of_slot):
    first = pair_of_slot
    second = M - 1 - pair_of_slot
    flip = first % 2 == 1
    even = jnp.where(flip, second, first)
    odd = jnp.where(flip, first, second)
    orders = jnp.stack([even, odd], 0).reshape(2, QLAT, 2).transpose(0, 2, 1).reshape(4, QLAT, 1)
    orders = jnp.broadcast_to(orders, (4, QLAT, 128))
    shape = jax.ShapeDtypeStruct((8, QLAT, HALF), BF16)
    out = pl.BlockSpec((2, QLAT, HALF), lambda i: (i, 0, 0))
    return pl.pallas_call(
        table_kernel,
        grid=(4,),
        in_specs=[pl.BlockSpec((1, QLAT, 128), lambda i: (i, 0, 0))],
        out_specs=(out, out),
        out_shape=(shape, shape),
        compiler_params=params(dimension_semantics=("arbitrary",)),
        cost_estimate=cost(5),
        name="tables",
    )(orders)


def to_grid(recv, t_hi, t_lo, z):
    for j in range(8):
        hi, lo = split(recv[:, j, :].T)
        for n in range(8):
            z[n, 16 * j : 16 * j + 16, :] = hi[16 * n : 16 * n + 16]
            z[n, 128 + 16 * j : 128 + 16 * j + 16, :] = lo[16 * n : 16 * n + 16]

    def block(nb):
        cols = slice(256 * nb, 256 * nb + 256)
        res = []
        for par in range(2):
            wide = jnp.zeros((256, 256), F32)
            narrow = jnp.zeros((128, 256), F32)
            for s in range(2):
                for p in range(2):
                    lhs = z[s * 4 + par * 2 + p]
                    n = par * 4 + s * 2 + p
                    wide = wide + mm(lhs, t_hi[n, :, cols])
                    narrow = narrow + mm(lhs[0:128], t_lo[n, :, cols])
            res.append(wide[0:128] + wide[128:256] + narrow)
        return res[0] + res[1], res[0] - res[1]

    return block


def fold(west, east, d, nb):
    cols = slice(256 * nb, 256 * nb + 256)
    for par, value in ((0, west + east), (1, west - east)):
        hi, lo = split(value)
        d[par, 0:128, cols] = hi
        d[par, 128:256, cols] = lo


def from_grid(d, t_hi, t_lo, res, out):
    for par in range(2):
        for s in range(2):
            for p in range(2):
                n = par * 4 + s * 2 + p
                wide = mm_t(d[par], t_hi[n])
                narrow = mm_t(d[par, 0:128], t_lo[n])
                res[s * 4 + par * 2 + p] = wide[0:128] + wide[128:256] + narrow
    for j in range(8):
        rows = jnp.concatenate([res[n, 16 * j : 16 * j + 16, :] for n in range(8)], axis=0)
        out[:, j, :] = rows.T


def wind_kernel(recv, t_hi, t_lo, out, wind, last, first, speed_ref, z, d, res, g):
    block = to_grid(recv, t_hi, t_lo, z)
    for nb in range(4):
        tend = []
        for side, value in enumerate(block(nb)):
            cols = slice(HALF * side + 256 * nb, HALF * side + 256 * nb + 256)
            for t in range(2):
                g[8 * side + 2 * nb + t] = value[:, 128 * t : 128 * t + 128]
            both = value.reshape(8, 16, 256)
            u, v = both[:, 0:8], both[:, 8:16]
            speed = jnp.sqrt(u * u + v * v + 1.0)
            speed_ref[:, cols] = speed.reshape(64, 256)
            drag = -DRAG_COEFFICIENT * speed
            tend.append(jnp.concatenate([drag * u, drag * v], axis=1).reshape(128, 256))
        fold(tend[0], tend[1], d, nb)
    for t in range(16):
        for l in range(TLEV):
            cols = slice(128 * t, 128 * t + 128)
            for n, value in (
                (l, g[t, pl.ds(l, 8, stride=16), :]),
                (TLEV + l, -g[t, pl.ds(8 + l, 8, stride=16), :]),
            ):
                wind[n, :, cols] = value
                last[n, :, cols] = value[4:8]
                first[n, :, cols] = value[0:4]
    from_grid(d, t_hi, t_lo, res, out)


def moist_kernel(recv, t_hi, t_lo, speed_ref, heat_ref, out, z, d, res):
    block = to_grid(recv, t_hi, t_lo, z)
    for nb in range(4):
        tend = []
        for side, value in enumerate(block(nb)):
            cols = slice(HALF * side + 256 * nb, HALF * side + 256 * nb + 256)
            both = value.reshape(8, 16, 256)
            t, q = both[:, 0:8], both[:, 8:16]
            speed = speed_ref[:, cols].reshape(8, 8, 256)
            n = 8 * side + 2 * nb
            heat = jnp.concatenate([heat_ref[n], heat_ref[n + 1]], axis=1).reshape(8, 8, 256)
            source = MOISTURE_SOURCE * t * q
            tend.append(
                jnp.concatenate(
                    [heat - source, source - RAINFALL_FACTOR * speed * q], axis=1
                ).reshape(128, 256)
            )
        fold(tend[0], tend[1], d, nb)
    from_grid(d, t_hi, t_lo, res, out)


FOURIER_SCRATCH = [
    pltpu.VMEM((8, 256, 256), BF16),
    pltpu.VMEM((2, 256, HALF), BF16),
    pltpu.VMEM((8, 128, 256), F32),
]


def wind_stage(recv, t_hi, t_lo):
    return pl.pallas_call(
        wind_kernel,
        out_shape=(
            jax.ShapeDtypeStruct((QLAT, 8, 128), F32),
            jax.ShapeDtypeStruct((2 * TLEV, 8, NLON), F32),
            jax.ShapeDtypeStruct((2 * TLEV, 4, NLON), F32),
            jax.ShapeDtypeStruct((2 * TLEV, 4, NLON), F32),
            jax.ShapeDtypeStruct((64, NLON), F32),
        ),
        scratch_shapes=FOURIER_SCRATCH + [pltpu.VMEM((16, 128, 128), F32)],
        compiler_params=params(),
        cost_estimate=cost(10),
        name="wind_stage",
    )(recv, t_hi, t_lo)


def moist_stage(recv, t_hi, t_lo, speed, heat):
    return pl.pallas_call(
        moist_kernel,
        out_shape=jax.ShapeDtypeStruct((QLAT, 8, 128), F32),
        scratch_shapes=FOURIER_SCRATCH,
        compiler_params=params(),
        cost_estimate=cost(10),
        name="moist_stage",
    )(recv, t_hi, t_lo, speed, heat)


def halo_of(above, below):
    return jnp.concatenate([below, above], axis=0)


def vertical(middle, halo, row):
    up_m, up_h = pltpu.roll(middle, 7, 0), pltpu.roll(halo, 7, 0)
    down_m, down_h = pltpu.roll(middle, 1, 0), pltpu.roll(halo, 1, 0)
    end, start = row == 7, row == 0
    return (
        (jnp.where(end, up_h, up_m), jnp.where(start, down_h, down_m)),
        (jnp.where(end, up_m, up_h), jnp.where(start, down_m, down_h)),
    )


def advect_kernel(
    rate, band, tracer, above, below, wind, wind_above, wind_below, out, heat, coef, total
):
    k = pl.program_id(0)
    row = lax.broadcasted_iota(jnp.int32, (8, 1), 0)

    @pl.when(k == 0)
    def _():
        for l in range(TLEV):
            m = TLEV + l
            u = (wind[l], halo_of(wind_above[l], wind_below[l]))
            w = (wind[m], halo_of(wind_above[m], wind_below[m]))
            moved = vertical(*w, row)
            faces = []
            for n, offset in ((0, row), (1, jnp.where(row < 4, row + 8, row - 8))):
                upper = band[0] * 8 + offset
                inside = (upper >= 0) & (upper <= NLAT - 2)
                faces.append(jnp.where(inside, 0.5 * (w[n] + moved[n][0]), 0.0))
            above_faces = vertical(*faces, row)
            for n in range(2):
                east = 0.5 * (u[n] + pltpu.roll(u[n], NLON - 1, 1))
                west = pltpu.roll(east, 1, 1)
                south, north = faces[n], above_faces[n][1]
                here = (
                    jnp.maximum(east, 0.0) - jnp.minimum(west, 0.0)
                    + jnp.maximum(south, 0.0) - jnp.minimum(north, 0.0)
                )
                stencil = (
                    -COURANT * here,
                    -COURANT * jnp.minimum(east, 0.0),
                    COURANT * jnp.maximum(west, 0.0),
                    -COURANT * jnp.minimum(south, 0.0),
                    COURANT * jnp.maximum(north, 0.0),
                )
                for c, value in enumerate(stencil):
                    coef[l, n, c] = value
        total[...] = jnp.zeros(total.shape, F32)

    def advect(field, l, parts):
        moved = vertical(*field, row)
        done = []
        for n in range(parts):
            q = field[n]
            south, north = moved[n]
            done.append(
                coef[l, n, 0] * q
                + coef[l, n, 1] * pltpu.roll(q, NLON - 1, 1)
                + coef[l, n, 2] * pltpu.roll(q, 1, 1)
                + coef[l, n, 3] * south
                + coef[l, n, 4] * north
            )
        return done

    for l in range(TLEV):
        q = (tracer[0, l], halo_of(above[0, l], below[0, l]))
        first = [a + b for a, b in zip(q, advect(q, l, 2))]
        second = [
            0.75 * a + 0.25 * (b + c) for a, b, c in zip(q, first, advect(first, l, 2))
        ]
        new = q[0] / 3.0 + 2.0 / 3.0 * (second[0] + advect(second, l, 1)[0])
        out[0, l] = new
        total[l] = total[l] + rate[k, l] * new

    @pl.when(k == NTR - 1)
    def _():
        heat[...] = jnp.zeros(heat.shape, F32)
        for t in range(16):
            for l in range(TLEV):
                heat[t, pl.ds(l, 8, stride=8), :] = total[l, :, 128 * t : 128 * t + 128]


def transport(rate, band, tracers, above, below, wind, wind_above, wind_below):
    block = pl.BlockSpec((1, TLEV, 8, NLON), lambda k, *_: (k, 0, 0, 0))
    edge = pl.BlockSpec((1, TLEV, 4, NLON), lambda k, *_: (k, 0, 0, 0))
    whole = pl.BlockSpec((2 * TLEV, 8, NLON), lambda k, *_: (0, 0, 0))
    side = pl.BlockSpec((2 * TLEV, 4, NLON), lambda k, *_: (0, 0, 0))
    return pl.pallas_call(
        advect_kernel,
        grid_spec=pltpu.PrefetchScalarGridSpec(
            num_scalar_prefetch=2,
            grid=(NTR,),
            in_specs=[block, edge, edge, whole, side, side],
            out_specs=(block, pl.BlockSpec((16, 64, 128), lambda k, *_: (0, 0, 0))),
            scratch_shapes=[
                pltpu.VMEM((TLEV, 2, 5, 8, NLON), F32),
                pltpu.VMEM((TLEV, 8, NLON), F32),
            ],
        ),
        out_shape=(
            jax.ShapeDtypeStruct((NTR, TLEV, 8, NLON), F32),
            jax.ShapeDtypeStruct((16, 64, 128), F32),
        ),
        compiler_params=params(dimension_semantics=("arbitrary",)),
        cost_estimate=cost(10),
        name="transport",
    )(rate, band, tracers, above, below, wind, wind_above, wind_below)


PART_ROWS = ALL_ROWS // 2


def tendency_kernel(
    pairs, place, recv, weight, hi_hbm, lo_hbm,
    own, ahead, far_a, far_b, behind, res, leg_hi, leg_lo, sem,
):
    step = pl.program_id(0)
    d = place[0]
    fetch(step, hi_hbm, lo_hbm, leg_hi, leg_lo, sem)
    lane = lax.broadcasted_iota(jnp.int32, (1, 128), 1)
    rhs = []
    bound = jnp.zeros((1, 128), jnp.int32)
    for b in range(4):
        lo_order = pairs[4 * step + b]
        f = recv[:, b // 2].reshape(QLAT, 128) * weight[...]
        even = pltpu.roll(f, (32 * b - 64 * (b % 2)) % 128, 1)
        odd = pltpu.roll(f, (32 * b - 64 * (b % 2) - 32) % 128, 1)
        here = lane // 32 == b
        flip = lo_order % 2 == 1
        low = jnp.where(here, jnp.where(flip, odd, even), 0.0)
        high = jnp.where(here, jnp.where(flip, even, odd), 0.0)
        rhs.append(split(jnp.concatenate([low, high], axis=1)))
        bound = jnp.where(here, M - lo_order, bound)
    rhs = jnp.concatenate([x for hi, lo in rhs for x in (hi, lo, hi)], axis=0)
    for part in range(2):
        rows = slice(PART_ROWS * part, PART_ROWS * (part + 1))
        lhs = []
        for b in range(4):
            hi = leg_hi[4 * step + b, rows, :]
            lhs += [hi, hi, leg_lo[4 * step + b, rows, :]]
        both = mm(jnp.concatenate(lhs, axis=1), rhs)
        r = PART_ROWS * part + lax.broadcasted_iota(jnp.int32, (PART_ROWS, 1), 0)
        value = jnp.where(r < bound, both[:, 0:128], both[:, 128:256])
        res[rows, :] = jnp.where(r <= M, value, 0.0)

    def get(k):
        return res[pl.ds(pl.multiple_of(((d + k) % 4) * ROWS, 8), ROWS), :]

    own[0] = get(0)
    ahead[0] = get(1)
    behind[0] = get(3)

    @pl.when(step < 2)
    def _():
        far_a[0] = get(2)

    @pl.when(step >= 2)
    def _():
        far_b[0] = get(2)


def tendency_sums(pairs, place, recv, weight, leg_hi, leg_lo):
    size = (1, ROWS, 128)
    block = pl.BlockSpec(size, lambda i, *_: (i, 0, 0))
    full = jax.ShapeDtypeStruct((4, ROWS, 128), F32)
    part = jax.ShapeDtypeStruct((2, ROWS, 128), F32)
    return pl.pallas_call(
        tendency_kernel,
        grid_spec=pltpu.PrefetchScalarGridSpec(
            num_scalar_prefetch=2,
            grid=(4,),
            in_specs=[
                pl.BlockSpec((32, 2, 8, 128), lambda i, *_: (0, i, 0, 0)),
                pl.BlockSpec((QLAT, 128), lambda i, *_: (0, 0)),
                ANY,
                ANY,
            ],
            out_specs=(
                block,
                block,
                pl.BlockSpec(size, lambda i, *_: (jnp.minimum(i, 1), 0, 0)),
                pl.BlockSpec(size, lambda i, *_: (jnp.maximum(i - 2, 0), 0, 0)),
                block,
            ),
            scratch_shapes=[pltpu.VMEM((ALL_ROWS, 128), F32)] + LEG_SCRATCH,
        ),
        out_shape=(full, full, part, part, full),
        compiler_params=params(dimension_semantics=("arbitrary",)),
        cost_estimate=cost(10),
        name="tendency_sums",
    )(pairs, place, recv, weight, leg_hi, leg_lo)


def unpack_kernel(a0, a1, a2, b0, b1, b2, out, scr):
    for ch, refs in ((0, (a0, a1, a2)), (1, (b0, b1, b2))):
        for g in range(4):
            scr[0:ROWS, :] = refs[0][g] + refs[1][g] + refs[2][g]
            value = scr[...].T
            for s in range(4):
                for p in range(2):
                    r0 = s * 32 + p * 16
                    c0 = p * 32 + ch * 16
                    out[4 * g + s, c0 : c0 + 16, :] = value[r0 : r0 + 16, 0:ROWS]


def unpack(pieces):
    return pl.pallas_call(
        unpack_kernel,
        out_shape=jax.ShapeDtypeStruct((SLOTS, 64, ROWS), F32),
        scratch_shapes=[pltpu.VMEM((384, 128), F32)],
        compiler_params=params(),
        cost_estimate=cost(4),
        name="unpack",
    )(*pieces)


def shift(x, axis, by):
    n = lax.axis_size(axis)
    return lax.ppermute(x, axis, [(i, (i + by) % n) for i in range(n)])


def neighbours(last, first):
    axes = ("ma", "pb")
    n = lax.axis_size("ma") * lax.axis_size("pb")
    down = [(i, i + 1) for i in range(n - 1)]
    return (
        lax.ppermute(last, axes, down),
        lax.ppermute(first, axes, [(b, a) for a, b in down]),
    )


def gather_rows(x):
    right = shift(x, "pb", 1)
    left = shift(x, "pb", -1)
    return right, left, shift(right[0:2], "pb", 1), shift(left[2:4], "pb", -1)


def scatter_rows(own, ahead, far_a, far_b, behind):
    via_a = shift(far_a, "pb", 1)
    via_b = shift(far_b, "pb", -1)
    ahead = jnp.concatenate([ahead[0:2] + via_a, ahead[2:4]], axis=0)
    behind = jnp.concatenate([behind[0:2], behind[2:4] + via_b], axis=0)
    return own, shift(ahead, "pb", 1), shift(behind, "pb", -1)


def exchange(x):
    return lax.all_to_all(x, "ma", 0, 0, tiled=True)


def shards(coefs, legendre, quad_weight, pair_of_slot, tracers, heat_rate):
    ma = lax.axis_index("ma")
    pb = lax.axis_index("pb")
    pairs = lax.dynamic_slice_in_dim(pair_of_slot, ma * SLOTS, SLOTS, 0)
    place = pb.reshape(1).astype(jnp.int32)
    band = (ma * lax.axis_size("pb") + pb).reshape(1).astype(jnp.int32)
    leg = legendre.reshape(SLOTS, 2 * ALL_ROWS, 128)
    weight = jnp.broadcast_to(quad_weight.reshape(QLAT, 1), (QLAT, 128))

    rows_a, rows_b = pack(jnp.transpose(coefs, (0, 2, 1)))
    got_a = gather_rows(rows_a)
    rows_b, near_a = lax.optimization_barrier((rows_b, got_a[0:2]))
    got_a = (*near_a, *got_a[2:])
    got_b = gather_rows(rows_b)
    t_hi, t_lo = fourier_tables(pair_of_slot)
    leg_hi, leg_lo = prepare(leg)
    sums_a = legendre_sums(pairs, place, rows_a, *got_a, leg_hi, leg_lo)
    sent_a = exchange(sums_a)
    above, below = neighbours(tracers[:, :, 4:8, :], tracers[:, :, 0:4, :])
    sums_b = legendre_sums(pairs, place, rows_b, *got_b, leg_hi, leg_lo)
    sent_b = exchange(sums_b)

    back_a, wind, last, first, speed = wind_stage(sent_a.reshape(QLAT, 8, 128), t_hi, t_lo)
    wind_above, wind_below = neighbours(last, first)
    back_a = exchange(back_a.reshape(32, 8, 8, 128))
    new_tracers, heat = transport(
        heat_rate, band, tracers, above, below, wind, wind_above, wind_below
    )
    back_b = moist_stage(sent_b.reshape(QLAT, 8, 128), t_hi, t_lo, speed, heat)
    back_b = exchange(back_b.reshape(32, 8, 8, 128))
    sums_a = tendency_sums(pairs, place, back_a, weight, leg_hi, leg_lo)
    sums_a = scatter_rows(*sums_a)
    sums_b = tendency_sums(pairs, place, back_b, weight, leg_hi, leg_lo)
    sums_b = scatter_rows(*sums_b)
    summed = unpack((*sums_a, *sums_b))
    return (jnp.transpose(summed, (0, 2, 1)), new_tracers)


def solution(mesh):
    in_specs = (
        P("ma", "pb", None),
        P("ma", None, "pb", None),
        P("pb", None),
        P(),
        P(None, None, ("ma", "pb"), None),
        P(),
    )
    out_specs = (P("ma", "pb", None), P(None, None, ("ma", "pb"), None))
    return jax.shard_map(shards, mesh=mesh, in_specs=in_specs, out_specs=out_specs, check_vma=False)
```

```python
import math

import jax
import jax.numpy as jnp
from jax import lax
from jax.experimental import pallas as pl
from jax.experimental.pallas import tpu as pltpu
from jax.sharding import PartitionSpec as P

M = 1024
NLAT = 1024
NLON = 2048
HALF = NLON // 2
NTR = 12
TLEV = 2
SLOTS = 16
ROWS = 264
ALL_ROWS = 1056
QLAT = 256

COURANT = 0.15
DRAG_COEFFICIENT = 0.2
MOISTURE_SOURCE = 0.3
RAINFALL_FACTOR = 0.2

BF16 = jnp.bfloat16
F32 = jnp.float32
VMEM_LIMIT = 28 * 1024 * 1024


def params(**kw):
    return pltpu.CompilerParams(vmem_limit_bytes=VMEM_LIMIT, **kw)


def cost(us):
    return pl.CostEstimate(flops=int(us * 2.5e8), bytes_accessed=1 << 20, transcendentals=0)


def split(x):
    hi = x.astype(BF16)
    return hi, (x - hi.astype(F32)).astype(BF16)


def mm(a, b):
    return lax.dot_general(a, b, (((1,), (0,)), ((), ())), preferred_element_type=F32)


def mm_t(a, b):
    return lax.dot_general(a, b, (((1,), (1,)), ((), ())), preferred_element_type=F32)


def pack_kernel(c_ref, a_ref, b_ref, scr):
    for ch, out in ((0, a_ref), (1, b_ref)):
        for g in range(4):
            for s in range(4):
                for p in range(2):
                    r0 = s * 32 + p * 16
                    c0 = p * 32 + ch * 16
                    scr[r0 : r0 + 16, 0:ROWS] = c_ref[4 * g + s, c0 : c0 + 16, :]
            out[g] = scr[...].T[0:ROWS]


def pack(coefs_t):
    shape = jax.ShapeDtypeStruct((4, ROWS, 128), F32)
    return pl.pallas_call(
        pack_kernel,
        out_shape=(shape, shape),
        scratch_shapes=[pltpu.VMEM((128, 384), F32)],
        compiler_params=params(),
        cost_estimate=cost(3),
        name="pack",
    )(coefs_t)


def legendre_kernel(
    pairs, place, own, right, left, far_a, far_b, hi_hbm, lo_hbm,
    out, rows, cols, leg_hi, leg_lo, sem,
):
    tables = (hi_hbm, lo_hbm, leg_hi, leg_lo, sem)
    start_tables(*tables)

    def body(step, carry):
        legendre_group(
            step, pairs, place, own, right, left, far_a, far_b, tables, out, rows, cols
        )
        return carry

    lax.fori_loop(0, 4, body, 0)


def legendre_group(
    step, pairs, place, own, right, left, far_a, far_b, tables, out, rows, cols
):
    _, _, leg_hi, leg_lo, _ = tables
    d = place[0]

    def put(k, value):
        start = pl.multiple_of(((d + k) % 4) * ROWS, 8)
        rows[pl.ds(start, ROWS), :] = value

    put(0, own[step])
    put(3, right[step])
    put(1, left[step])
    put(2, jnp.where(step < 2, far_a[jnp.minimum(step, 1)], far_b[jnp.maximum(step - 2, 0)]))
    cols[...] = rows[...].T
    for q in range(4):
        next_tables(4 * step + q, *tables)
    sums = []
    for q in range(4):
        lo_order = pairs[4 * step + q]
        n = (4 * step + q) % RING
        odd = lo_order % 2
        x = cols[32 * q : 32 * q + 32, 0:M]
        r = lax.broadcasted_iota(jnp.int32, (1, M), 1)
        low = (r < M - lo_order).astype(jnp.int32)
        weight = jnp.where((low == 1) & (lo_order == 0), 1.0, 2.0)
        in_even = low != odd
        x = x * weight
        lhs = jnp.concatenate([jnp.where(in_even, x, 0.0), jnp.where(in_even, 0.0, x)], axis=0)
        hi, lo = split(lhs)
        both = jnp.concatenate([hi, lo], axis=0)
        last = 2.0 * cols[32 * q : 32 * q + 32, M : M + 128][:, 0:1]
        row = leg_hi[n, M : M + 16, :].astype(F32)[0:1] + leg_lo[n, M : M + 16, :].astype(F32)[0:1]
        outer = last * row
        first = mm(both, leg_hi[n, 0:M, :])
        acc = first[0:64] + first[64:128] + mm(hi, leg_lo[n, 0:M, :])
        sums.append(
            acc
            + jnp.concatenate(
                [jnp.where(odd == 1, outer, 0.0), jnp.where(odd == 1, 0.0, outer)], axis=0
            )
        )
    for p in range(2):
        out[:, 2 * step + p] = jnp.concatenate(sums[2 * p : 2 * p + 2], axis=0).T.reshape(32, 8, 128)


DEPTH = 4


def prepare_kernel(leg, hi_out, lo_out, raw, hi_buf, lo_buf, load_sem, store_sem):
    def load(n):
        slot = n % DEPTH
        return pltpu.make_async_copy(leg.at[n], raw.at[slot], load_sem.at[slot])

    def store(n):
        slot = n % DEPTH
        return (
            pltpu.make_async_copy(hi_buf.at[slot], hi_out.at[n], store_sem.at[0, slot]),
            pltpu.make_async_copy(lo_buf.at[slot], lo_out.at[n], store_sem.at[1, slot]),
        )

    for n in range(DEPTH):
        load(n).start()

    def body(n, carry):
        load(n).wait()

        @pl.when(n >= DEPTH)
        def _():
            for copy in store(n - DEPTH):
                copy.wait()

        slot = n % DEPTH
        for t in range(2):
            hi, lo = split(raw[slot, pl.ds(t, ALL_ROWS, stride=2), :])
            hi_buf[slot, :, 128 * t : 128 * t + 128] = hi
            lo_buf[slot, :, 128 * t : 128 * t + 128] = lo
        for copy in store(n):
            copy.start()

        @pl.when(n + DEPTH < SLOTS)
        def _():
            load(n + DEPTH).start()

        return carry

    lax.fori_loop(0, SLOTS, body, 0)
    for n in range(SLOTS - DEPTH, SLOTS):
        for copy in store(n):
            copy.wait()


ANY = pl.BlockSpec(memory_space=pl.ANY)
ON_CHIP = pl.BlockSpec(memory_space=pltpu.VMEM)
SCALARS = pl.BlockSpec(memory_space=pltpu.SMEM)


def prepare(leg):
    shape = pltpu.HBM((SLOTS, ALL_ROWS, QLAT), BF16)
    buffer = pltpu.VMEM((DEPTH, ALL_ROWS, QLAT), BF16)
    return pl.pallas_call(
        prepare_kernel,
        in_specs=[ANY],
        out_specs=(ANY, ANY),
        out_shape=(shape, shape),
        scratch_shapes=[
            pltpu.VMEM((DEPTH, 2 * ALL_ROWS, 128), F32),
            buffer,
            buffer,
            pltpu.SemaphoreType.DMA((DEPTH,)),
            pltpu.SemaphoreType.DMA((2, DEPTH)),
        ],
        compiler_params=params(),
        cost_estimate=cost(11),
        name="prepare",
    )(in_hbm(leg))


def in_hbm(x):
    return pltpu.with_memory_space_constraint(x, pltpu.HBM)


RING = 12
AHEAD = 8
LEG_SCRATCH = [
    pltpu.VMEM((RING, ALL_ROWS, QLAT), BF16),
    pltpu.VMEM((RING, ALL_ROWS, QLAT), BF16),
    pltpu.SemaphoreType.DMA((2, RING)),
]


def slot_tables(n, hi_hbm, lo_hbm, leg_hi, leg_lo, sem):
    slot = n % RING
    return (
        pltpu.make_async_copy(hi_hbm.at[n], leg_hi.at[slot], sem.at[0, slot]),
        pltpu.make_async_copy(lo_hbm.at[n], leg_lo.at[slot], sem.at[1, slot]),
    )


def start_tables(*refs):
    for n in range(AHEAD):
        for copy in slot_tables(n, *refs):
            copy.start()


def next_tables(n, *refs):
    for copy in slot_tables(n, *refs):
        copy.wait()

    @pl.when(n + AHEAD < SLOTS)
    def _():
        for copy in slot_tables(n + AHEAD, *refs):
            copy.start()


def legendre_sums(pairs, place, own, right, left, far_a, far_b, leg_hi, leg_lo):
    return pl.pallas_call(
        legendre_kernel,
        in_specs=[SCALARS] * 2 + [ON_CHIP] * 5 + [ANY] * 2,
        out_specs=ON_CHIP,
        out_shape=jax.ShapeDtypeStruct((32, 8, 8, 128), F32),
        scratch_shapes=[pltpu.VMEM((1152, 128), F32), pltpu.VMEM((128, 1152), F32)] + LEG_SCRATCH,
        compiler_params=params(),
        cost_estimate=cost(10),
        name="legendre_sums",
    )(pairs, place, own, right, left, far_a, far_b, in_hbm(leg_hi), in_hbm(leg_lo))


def cos_sin(phase):
    quadrant = (phase + NLON // 8) >> 9
    x = (phase - (quadrant << 9)).astype(F32) * (2.0 * math.pi / NLON)
    y = x * x
    s = x * (1.0 + y * (-1 / 6 + y * (1 / 120 + y * (-1 / 5040 + y * (1 / 362880)))))
    c = 1.0 + y * (-1 / 2 + y * (1 / 24 + y * (-1 / 720 + y * (1 / 40320 + y * (-1 / 3628800)))))
    swap = (quadrant & 1) == 1
    cos = jnp.where(swap, s, c)
    sin = jnp.where(swap, c, s)
    cos = jnp.where(((quadrant + 1) & 2) != 0, -cos, cos)
    return cos, jnp.where((quadrant & 2) != 0, -sin, sin)


def table_kernel(orders, hi_out, lo_out, hi_buf, lo_buf, sem):
    def stores(n):
        rows = pl.ds(2 * n, 2)
        return (
            pltpu.make_async_copy(hi_buf.at[rows], hi_out.at[rows], sem.at[0, n]),
            pltpu.make_async_copy(lo_buf.at[rows], lo_out.at[rows], sem.at[1, n]),
        )

    def body(n, carry):
        table_pair(n, orders, hi_buf, lo_buf)
        for copy in stores(n):
            copy.start()
        return carry

    lax.fori_loop(0, 4, body, 0)
    for n in range(4):
        for copy in stores(n):
            copy.wait()


TABLE = pltpu.VMEM((8, QLAT, HALF), BF16)


def table_pair(n, orders, hi_ref, lo_ref):
    m = orders[n]
    product = m * lax.broadcasted_iota(jnp.int32, (1, 128), 1)
    cb, sb = cos_sin(product & (NLON - 1))
    factor = 1.0 / math.sqrt(NLON)
    cb, sb = cb * factor, sb * factor
    ca, sa = cos_sin((product & 15) << 7)
    for a in range(8):
        c1, s1 = ca[:, a : a + 1], sa[:, a : a + 1]
        for part, value in ((0, c1 * cb - s1 * sb), (1, -(s1 * cb + c1 * sb))):
            hi, lo = split(value)
            hi_ref[2 * n + part, :, 128 * a : 128 * a + 128] = hi
            lo_ref[2 * n + part, :, 128 * a : 128 * a + 128] = lo


def fourier_tables(pair_of_slot):
    first = pair_of_slot
    second = M - 1 - pair_of_slot
    flip = first % 2 == 1
    even = jnp.where(flip, second, first)
    odd = jnp.where(flip, first, second)
    orders = jnp.stack([even, odd], 0).reshape(2, QLAT, 2).transpose(0, 2, 1).reshape(4, QLAT, 1)
    orders = jnp.broadcast_to(orders, (4, QLAT, 128))
    shape = pltpu.HBM((8, QLAT, HALF), BF16)
    return pl.pallas_call(
        table_kernel,
        in_specs=[ON_CHIP],
        out_specs=(ANY, ANY),
        out_shape=(shape, shape),
        scratch_shapes=[TABLE, TABLE, pltpu.SemaphoreType.DMA((2, 4))],
        compiler_params=params(),
        cost_estimate=cost(5),
        name="tables",
    )(orders)


def table_loads(hi_hbm, lo_hbm, t_hi, t_lo, sem, nb):
    cols = pl.ds(256 * nb, 256)
    return (
        pltpu.make_async_copy(hi_hbm.at[:, :, cols], t_hi.at[:, :, cols], sem.at[0, nb]),
        pltpu.make_async_copy(lo_hbm.at[:, :, cols], t_lo.at[:, :, cols], sem.at[1, nb]),
    )


def to_grid(recv, hi_hbm, lo_hbm, t_hi, t_lo, sem, z):
    for nb in range(4):
        for copy in table_loads(hi_hbm, lo_hbm, t_hi, t_lo, sem, nb):
            copy.start()
    for j in range(8):
        hi, lo = split(recv[:, j, :].T)
        for n in range(8):
            z[n, 16 * j : 16 * j + 16, :] = hi[16 * n : 16 * n + 16]
            z[n, 128 + 16 * j : 128 + 16 * j + 16, :] = lo[16 * n : 16 * n + 16]

    def block(nb):
        cols = slice(256 * nb, 256 * nb + 256)
        for copy in table_loads(hi_hbm, lo_hbm, t_hi, t_lo, sem, nb):
            copy.wait()
        res = []
        for par in range(2):
            wide = jnp.zeros((256, 256), F32)
            narrow = jnp.zeros((128, 256), F32)
            for s in range(2):
                for p in range(2):
                    lhs = z[s * 4 + par * 2 + p]
                    n = par * 4 + s * 2 + p
                    wide = wide + mm(lhs, t_hi[n, :, cols])
                    narrow = narrow + mm(lhs[0:128], t_lo[n, :, cols])
            res.append(wide[0:128] + wide[128:256] + narrow)
        return res[0] + res[1], res[0] - res[1]

    return block


def fold(west, east, d, nb):
    cols = slice(256 * nb, 256 * nb + 256)
    for par, value in ((0, west + east), (1, west - east)):
        hi, lo = split(value)
        d[par, 0:128, cols] = hi
        d[par, 128:256, cols] = lo


def from_grid(d, t_hi, t_lo, res, out):
    for par in range(2):
        for s in range(2):
            for p in range(2):
                n = par * 4 + s * 2 + p
                wide = mm_t(d[par], t_hi[n])
                narrow = mm_t(d[par, 0:128], t_lo[n])
                res[s * 4 + par * 2 + p] = wide[0:128] + wide[128:256] + narrow
    for j in range(8):
        rows = jnp.concatenate([res[n, 16 * j : 16 * j + 16, :] for n in range(8)], axis=0)
        out[:, j, :] = rows.T


def wind_kernel(
    recv, hi_hbm, lo_hbm, out, wind, last, first, speed_ref, z, d, res, t_hi, t_lo, sem, g
):
    block = to_grid(recv, hi_hbm, lo_hbm, t_hi, t_lo, sem, z)
    for nb in range(4):
        tend = []
        for side, value in enumerate(block(nb)):
            cols = slice(HALF * side + 256 * nb, HALF * side + 256 * nb + 256)
            for t in range(2):
                g[8 * side + 2 * nb + t] = value[:, 128 * t : 128 * t + 128]
            both = value.reshape(8, 16, 256)
            u, v = both[:, 0:8], both[:, 8:16]
            speed = jnp.sqrt(u * u + v * v + 1.0)
            speed_ref[:, cols] = speed.reshape(64, 256)
            drag = -DRAG_COEFFICIENT * speed
            tend.append(jnp.concatenate([drag * u, drag * v], axis=1).reshape(128, 256))
        fold(tend[0], tend[1], d, nb)
    for t in range(16):
        for l in range(TLEV):
            cols = slice(128 * t, 128 * t + 128)
            for n, value in (
                (l, g[t, pl.ds(l, 8, stride=16), :]),
                (TLEV + l, -g[t, pl.ds(8 + l, 8, stride=16), :]),
            ):
                wind[n, :, cols] = value
                last[n, :, cols] = value[4:8]
                first[n, :, cols] = value[0:4]
    from_grid(d, t_hi, t_lo, res, out)


def moist_kernel(
    recv, hi_hbm, lo_hbm, speed_ref, heat_ref, out, z, d, res, t_hi, t_lo, sem
):
    block = to_grid(recv, hi_hbm, lo_hbm, t_hi, t_lo, sem, z)
    for nb in range(4):
        tend = []
        for side, value in enumerate(block(nb)):
            cols = slice(HALF * side + 256 * nb, HALF * side + 256 * nb + 256)
            both = value.reshape(8, 16, 256)
            t, q = both[:, 0:8], both[:, 8:16]
            speed = speed_ref[:, cols].reshape(8, 8, 256)
            n = 8 * side + 2 * nb
            heat = jnp.concatenate([heat_ref[n], heat_ref[n + 1]], axis=1).reshape(8, 8, 256)
            source = MOISTURE_SOURCE * t * q
            tend.append(
                jnp.concatenate(
                    [heat - source, source - RAINFALL_FACTOR * speed * q], axis=1
                ).reshape(128, 256)
            )
        fold(tend[0], tend[1], d, nb)
    from_grid(d, t_hi, t_lo, res, out)


FOURIER_SCRATCH = [
    pltpu.VMEM((8, 256, 256), BF16),
    pltpu.VMEM((2, 256, HALF), BF16),
    pltpu.VMEM((8, 128, 256), F32),
    TABLE,
    TABLE,
    pltpu.SemaphoreType.DMA((2, 4)),
]


def wind_stage(recv, t_hi, t_lo):
    return pl.pallas_call(
        wind_kernel,
        in_specs=[ON_CHIP, ANY, ANY],
        out_shape=(
            jax.ShapeDtypeStruct((QLAT, 8, 128), F32),
            jax.ShapeDtypeStruct((2 * TLEV, 8, NLON), F32),
            jax.ShapeDtypeStruct((2 * TLEV, 4, NLON), F32),
            jax.ShapeDtypeStruct((2 * TLEV, 4, NLON), F32),
            jax.ShapeDtypeStruct((64, NLON), F32),
        ),
        scratch_shapes=FOURIER_SCRATCH + [pltpu.VMEM((16, 128, 128), F32)],
        compiler_params=params(),
        cost_estimate=cost(10),
        name="wind_stage",
    )(recv, in_hbm(t_hi), in_hbm(t_lo))


def moist_stage(recv, t_hi, t_lo, speed, heat):
    return pl.pallas_call(
        moist_kernel,
        in_specs=[ON_CHIP, ANY, ANY, ON_CHIP, ON_CHIP],
        out_shape=jax.ShapeDtypeStruct((QLAT, 8, 128), F32),
        scratch_shapes=FOURIER_SCRATCH,
        compiler_params=params(),
        cost_estimate=cost(10),
        name="moist_stage",
    )(recv, in_hbm(t_hi), in_hbm(t_lo), speed, heat)


def halo_of(above, below):
    return jnp.concatenate([below, above], axis=0)


def vertical(middle, halo, row):
    up_m, up_h = pltpu.roll(middle, 7, 0), pltpu.roll(halo, 7, 0)
    down_m, down_h = pltpu.roll(middle, 1, 0), pltpu.roll(halo, 1, 0)
    end, start = row == 7, row == 0
    return (
        (jnp.where(end, up_h, up_m), jnp.where(start, down_h, down_m)),
        (jnp.where(end, up_m, up_h), jnp.where(start, down_m, down_h)),
    )


def advect_kernel(
    rate, band, tracer, above, below, wind, wind_above, wind_below, out, heat, coef, total
):
    k = pl.program_id(0)
    row = lax.broadcasted_iota(jnp.int32, (8, 1), 0)

    @pl.when(k == 0)
    def _():
        for l in range(TLEV):
            m = TLEV + l
            u = (wind[l], halo_of(wind_above[l], wind_below[l]))
            w = (wind[m], halo_of(wind_above[m], wind_below[m]))
            moved = vertical(*w, row)
            faces = []
            for n, offset in ((0, row), (1, jnp.where(row < 4, row + 8, row - 8))):
                upper = band[0] * 8 + offset
                inside = (upper >= 0) & (upper <= NLAT - 2)
                faces.append(jnp.where(inside, 0.5 * (w[n] + moved[n][0]), 0.0))
            above_faces = vertical(*faces, row)
            for n in range(2):
                east = 0.5 * (u[n] + pltpu.roll(u[n], NLON - 1, 1))
                west = pltpu.roll(east, 1, 1)
                south, north = faces[n], above_faces[n][1]
                here = (
                    jnp.maximum(east, 0.0) - jnp.minimum(west, 0.0)
                    + jnp.maximum(south, 0.0) - jnp.minimum(north, 0.0)
                )
                stencil = (
                    -COURANT * here,
                    -COURANT * jnp.minimum(east, 0.0),
                    COURANT * jnp.maximum(west, 0.0),
                    -COURANT * jnp.minimum(south, 0.0),
                    COURANT * jnp.maximum(north, 0.0),
                )
                for c, value in enumerate(stencil):
                    coef[l, n, c] = value
        total[...] = jnp.zeros(total.shape, F32)

    def advect(field, l, parts):
        moved = vertical(*field, row)
        done = []
        for n in range(parts):
            q = field[n]
            south, north = moved[n]
            done.append(
                coef[l, n, 0] * q
                + coef[l, n, 1] * pltpu.roll(q, NLON - 1, 1)
                + coef[l, n, 2] * pltpu.roll(q, 1, 1)
                + coef[l, n, 3] * south
                + coef[l, n, 4] * north
            )
        return done

    for l in range(TLEV):
        q = (tracer[0, l], halo_of(above[0, l], below[0, l]))
        first = [a + b for a, b in zip(q, advect(q, l, 2))]
        second = [
            0.75 * a + 0.25 * (b + c) for a, b, c in zip(q, first, advect(first, l, 2))
        ]
        new = q[0] / 3.0 + 2.0 / 3.0 * (second[0] + advect(second, l, 1)[0])
        out[0, l] = new
        total[l] = total[l] + rate[k, l] * new

    @pl.when(k == NTR - 1)
    def _():
        heat[...] = jnp.zeros(heat.shape, F32)
        for t in range(16):
            for l in range(TLEV):
                heat[t, pl.ds(l, 8, stride=8), :] = total[l, :, 128 * t : 128 * t + 128]


def transport(rate, band, tracers, above, below, wind, wind_above, wind_below):
    block = pl.BlockSpec((1, TLEV, 8, NLON), lambda k, *_: (k, 0, 0, 0))
    edge = pl.BlockSpec((1, TLEV, 4, NLON), lambda k, *_: (k, 0, 0, 0))
    whole = pl.BlockSpec((2 * TLEV, 8, NLON), lambda k, *_: (0, 0, 0))
    side = pl.BlockSpec((2 * TLEV, 4, NLON), lambda k, *_: (0, 0, 0))
    return pl.pallas_call(
        advect_kernel,
        grid_spec=pltpu.PrefetchScalarGridSpec(
            num_scalar_prefetch=2,
            grid=(NTR,),
            in_specs=[block, edge, edge, whole, side, side],
            out_specs=(block, pl.BlockSpec((16, 64, 128), lambda k, *_: (0, 0, 0))),
            scratch_shapes=[
                pltpu.VMEM((TLEV, 2, 5, 8, NLON), F32),
                pltpu.VMEM((TLEV, 8, NLON), F32),
            ],
        ),
        out_shape=(
            jax.ShapeDtypeStruct((NTR, TLEV, 8, NLON), F32),
            jax.ShapeDtypeStruct((16, 64, 128), F32),
        ),
        compiler_params=params(dimension_semantics=("arbitrary",)),
        cost_estimate=cost(10),
        name="transport",
    )(rate, band, tracers, above, below, wind, wind_above, wind_below)


PART_ROWS = ALL_ROWS // 2


def tendency_kernel(
    pairs, place, recv, weight, hi_hbm, lo_hbm,
    own, ahead, far_a, far_b, behind, res, leg_hi, leg_lo, sem,
):
    tables = (hi_hbm, lo_hbm, leg_hi, leg_lo, sem)
    start_tables(*tables)

    def body(step, carry):
        tendency_group(
            step, pairs, place, recv, weight, tables, own, ahead, far_a, far_b, behind, res
        )
        return carry

    lax.fori_loop(0, 4, body, 0)


def tendency_group(
    step, pairs, place, recv, weight, tables, own, ahead, far_a, far_b, behind, res
):
    _, _, leg_hi, leg_lo, _ = tables
    d = place[0]
    lane = lax.broadcasted_iota(jnp.int32, (1, 128), 1)
    rhs = []
    bound = jnp.zeros((1, 128), jnp.int32)
    for b in range(4):
        lo_order = pairs[4 * step + b]
        f = recv[:, 2 * step + b // 2].reshape(QLAT, 128) * weight[...]
        even = pltpu.roll(f, (32 * b - 64 * (b % 2)) % 128, 1)
        odd = pltpu.roll(f, (32 * b - 64 * (b % 2) - 32) % 128, 1)
        here = lane // 32 == b
        flip = lo_order % 2 == 1
        low = jnp.where(here, jnp.where(flip, odd, even), 0.0)
        high = jnp.where(here, jnp.where(flip, even, odd), 0.0)
        rhs.append(split(jnp.concatenate([low, high], axis=1)))
        bound = jnp.where(here, M - lo_order, bound)
    rhs = jnp.concatenate([x for hi, lo in rhs for x in (hi, lo, hi)], axis=0)
    for b in range(4):
        next_tables(4 * step + b, *tables)
    for part in range(2):
        rows = slice(PART_ROWS * part, PART_ROWS * (part + 1))
        lhs = []
        for b in range(4):
            n = (4 * step + b) % RING
            hi = leg_hi[n, rows, :]
            lhs += [hi, hi, leg_lo[n, rows, :]]
        both = mm(jnp.concatenate(lhs, axis=1), rhs)
        r = PART_ROWS * part + lax.broadcasted_iota(jnp.int32, (PART_ROWS, 1), 0)
        value = jnp.where(r < bound, both[:, 0:128], both[:, 128:256])
        res[rows, :] = jnp.where(r <= M, value, 0.0)

    def get(k):
        return res[pl.ds(pl.multiple_of(((d + k) % 4) * ROWS, 8), ROWS), :]

    own[step] = get(0)
    ahead[step] = get(1)
    behind[step] = get(3)

    @pl.when(step < 2)
    def _():
        far_a[step] = get(2)

    @pl.when(step >= 2)
    def _():
        far_b[step - 2] = get(2)


def tendency_sums(pairs, place, recv, weight, leg_hi, leg_lo):
    full = jax.ShapeDtypeStruct((4, ROWS, 128), F32)
    part = jax.ShapeDtypeStruct((2, ROWS, 128), F32)
    return pl.pallas_call(
        tendency_kernel,
        in_specs=[SCALARS] * 2 + [ON_CHIP] * 2 + [ANY] * 2,
        out_specs=(ON_CHIP,) * 5,
        out_shape=(full, full, part, part, full),
        scratch_shapes=[pltpu.VMEM((ALL_ROWS, 128), F32)] + LEG_SCRATCH,
        compiler_params=params(),
        cost_estimate=cost(10),
        name="tendency_sums",
    )(pairs, place, recv, weight, in_hbm(leg_hi), in_hbm(leg_lo))


def unpack_kernel(a0, a1, a2, b0, b1, b2, out, scr):
    for ch, refs in ((0, (a0, a1, a2)), (1, (b0, b1, b2))):
        for g in range(4):
            scr[0:ROWS, :] = refs[0][g] + refs[1][g] + refs[2][g]
            value = scr[...].T
            for s in range(4):
                for p in range(2):
                    r0 = s * 32 + p * 16
                    c0 = p * 32 + ch * 16
                    out[4 * g + s, c0 : c0 + 16, :] = value[r0 : r0 + 16, 0:ROWS]


def unpack(pieces):
    return pl.pallas_call(
        unpack_kernel,
        out_shape=jax.ShapeDtypeStruct((SLOTS, 64, ROWS), F32),
        scratch_shapes=[pltpu.VMEM((384, 128), F32)],
        compiler_params=params(),
        cost_estimate=cost(4),
        name="unpack",
    )(*pieces)


def shift(x, axis, by):
    n = lax.axis_size(axis)
    return lax.ppermute(x, axis, [(i, (i + by) % n) for i in range(n)])


def neighbours(last, first):
    axes = ("ma", "pb")
    n = lax.axis_size("ma") * lax.axis_size("pb")
    down = [(i, i + 1) for i in range(n - 1)]
    return (
        lax.ppermute(last, axes, down),
        lax.ppermute(first, axes, [(b, a) for a, b in down]),
    )


def gather_rows(x):
    right = shift(x, "pb", 1)
    left = shift(x, "pb", -1)
    return right, left, shift(right[0:2], "pb", 1), shift(left[2:4], "pb", -1)


def scatter_rows(own, ahead, far_a, far_b, behind):
    via_a = shift(far_a, "pb", 1)
    via_b = shift(far_b, "pb", -1)
    ahead = jnp.concatenate([ahead[0:2] + via_a, ahead[2:4]], axis=0)
    behind = jnp.concatenate([behind[0:2], behind[2:4] + via_b], axis=0)
    return own, shift(ahead, "pb", 1), shift(behind, "pb", -1)


def exchange(x):
    return lax.all_to_all(x, "ma", 0, 0, tiled=True)


def shards(coefs, legendre, quad_weight, pair_of_slot, tracers, heat_rate):
    ma = lax.axis_index("ma")
    pb = lax.axis_index("pb")
    pairs = lax.dynamic_slice_in_dim(pair_of_slot, ma * SLOTS, SLOTS, 0)
    place = pb.reshape(1).astype(jnp.int32)
    band = (ma * lax.axis_size("pb") + pb).reshape(1).astype(jnp.int32)
    leg = legendre.reshape(SLOTS, 2 * ALL_ROWS, 128)
    weight = jnp.broadcast_to(quad_weight.reshape(QLAT, 1), (QLAT, 128))

    rows_a, rows_b = pack(jnp.transpose(coefs, (0, 2, 1)))
    got_a = gather_rows(rows_a)
    rows_b, near_a = lax.optimization_barrier((rows_b, got_a[0:2]))
    got_a = (*near_a, *got_a[2:])
    got_b = gather_rows(rows_b)
    t_hi, t_lo = fourier_tables(pair_of_slot)
    leg_hi, leg_lo = prepare(leg)
    sums_a = legendre_sums(pairs, place, rows_a, *got_a, leg_hi, leg_lo)
    sent_a = exchange(sums_a)
    above, below = neighbours(tracers[:, :, 4:8, :], tracers[:, :, 0:4, :])
    sums_b = legendre_sums(pairs, place, rows_b, *got_b, leg_hi, leg_lo)
    sent_b = exchange(sums_b)

    back_a, wind, last, first, speed = wind_stage(sent_a.reshape(QLAT, 8, 128), t_hi, t_lo)
    wind_above, wind_below = neighbours(last, first)
    back_a = exchange(back_a.reshape(32, 8, 8, 128))
    new_tracers, heat = transport(
        heat_rate, band, tracers, above, below, wind, wind_above, wind_below
    )
    back_b = moist_stage(sent_b.reshape(QLAT, 8, 128), t_hi, t_lo, speed, heat)
    back_b = exchange(back_b.reshape(32, 8, 8, 128))
    sums_a = tendency_sums(pairs, place, back_a, weight, leg_hi, leg_lo)
    sums_a = scatter_rows(*sums_a)
    sums_b = tendency_sums(pairs, place, back_b, weight, leg_hi, leg_lo)
    sums_b = scatter_rows(*sums_b)
    summed = unpack((*sums_a, *sums_b))
    return (jnp.transpose(summed, (0, 2, 1)), new_tracers)


def solution(mesh):
    in_specs = (
        P("ma", "pb", None),
        P("ma", None, "pb", None),
        P("pb", None),
        P(),
        P(None, None, ("ma", "pb"), None),
        P(),
    )
    out_specs = (P("ma", "pb", None), P(None, None, ("ma", "pb"), None))
    return jax.shard_map(shards, mesh=mesh, in_specs=in_specs, out_specs=out_specs, check_vma=False)
```

```python
import functools
import math

import jax
import jax.numpy as jnp
from jax import lax
from jax.experimental import pallas as pl
from jax.experimental.pallas import tpu as pltpu
from jax.sharding import PartitionSpec as P

M = 1024
NLAT = 1024
NLON = 2048
HALF = NLON // 2
NTR = 12
TLEV = 2
SLOTS = 16
ROWS = 264
ALL_ROWS = 1056
QLAT = 256

COURANT = 0.15
DRAG_COEFFICIENT = 0.2
MOISTURE_SOURCE = 0.3
RAINFALL_FACTOR = 0.2

BF16 = jnp.bfloat16
F32 = jnp.float32
VMEM_LIMIT = 28 * 1024 * 1024


def params(**kw):
    return pltpu.CompilerParams(vmem_limit_bytes=VMEM_LIMIT, **kw)


def cost(us):
    return pl.CostEstimate(flops=int(us * 2.5e8), bytes_accessed=1 << 20, transcendentals=0)


def split(x):
    hi = x.astype(BF16)
    return hi, (x - hi.astype(F32)).astype(BF16)


def mm(a, b):
    return lax.dot_general(a, b, (((1,), (0,)), ((), ())), preferred_element_type=F32)


def mm_t(a, b):
    return lax.dot_general(a, b, (((1,), (1,)), ((), ())), preferred_element_type=F32)


def pack_kernel(c_ref, a_ref, b_ref, scr):
    for ch, out in ((0, a_ref), (1, b_ref)):
        for g in range(4):
            for s in range(4):
                for p in range(2):
                    r0 = s * 32 + p * 16
                    c0 = p * 32 + ch * 16
                    scr[r0 : r0 + 16, 0:ROWS] = c_ref[4 * g + s, c0 : c0 + 16, :]
            out[g] = scr[...].T[0:ROWS]


def pack(coefs_t):
    shape = jax.ShapeDtypeStruct((4, ROWS, 128), F32)
    return pl.pallas_call(
        pack_kernel,
        out_shape=(shape, shape),
        scratch_shapes=[pltpu.VMEM((128, 384), F32)],
        compiler_params=params(),
        cost_estimate=cost(3),
        name="pack",
    )(coefs_t)


def legendre_kernel(
    pairs, place, own, right, left, far_a, far_b, hi_hbm, lo_hbm,
    out, rows, cols, leg_hi, leg_lo, sem,
):
    tables = (hi_hbm, lo_hbm, leg_hi, leg_lo, sem)
    start_tables(AHEAD, *tables)

    def body(step, carry):
        legendre_group(
            step, pairs, place, own, right, left, far_a, far_b, tables, out, rows, cols
        )
        return carry

    lax.fori_loop(0, 4, body, 0)


def legendre_group(
    step, pairs, place, own, right, left, far_a, far_b, tables, out, rows, cols
):
    _, _, leg_hi, leg_lo, _ = tables
    d = place[0]

    def put(k, value):
        start = pl.multiple_of(((d + k) % 4) * ROWS, 8)
        rows[pl.ds(start, ROWS), :] = value

    put(0, own[step])
    put(3, right[step])
    put(1, left[step])
    put(2, jnp.where(step < 2, far_a[jnp.minimum(step, 1)], far_b[jnp.maximum(step - 2, 0)]))
    cols[...] = rows[...].T
    for q in range(4):
        next_tables(4 * step + q, AHEAD, SLOTS, *tables)
    sums = []
    for q in range(4):
        lo_order = pairs[4 * step + q]
        n = (4 * step + q) % RING
        odd = lo_order % 2
        x = cols[32 * q : 32 * q + 32, 0:M]
        r = lax.broadcasted_iota(jnp.int32, (1, M), 1)
        low = (r < M - lo_order).astype(jnp.int32)
        weight = jnp.where((low == 1) & (lo_order == 0), 1.0, 2.0)
        in_even = low != odd
        x = x * weight
        lhs = jnp.concatenate([jnp.where(in_even, x, 0.0), jnp.where(in_even, 0.0, x)], axis=0)
        hi, lo = split(lhs)
        both = jnp.concatenate([hi, lo], axis=0)
        last = 2.0 * cols[32 * q : 32 * q + 32, M : M + 128][:, 0:1]
        row = leg_hi[n, M : M + 16, :].astype(F32)[0:1] + leg_lo[n, M : M + 16, :].astype(F32)[0:1]
        outer = last * row
        first = mm(both, leg_hi[n, 0:M, :])
        acc = first[0:64] + first[64:128] + mm(hi, leg_lo[n, 0:M, :])
        sums.append(
            acc
            + jnp.concatenate(
                [jnp.where(odd == 1, outer, 0.0), jnp.where(odd == 1, 0.0, outer)], axis=0
            )
        )
    for p in range(2):
        out[:, 2 * step + p] = jnp.concatenate(sums[2 * p : 2 * p + 2], axis=0).T.reshape(32, 8, 128)


DEPTH = 4


def prepare_kernel(leg, hi_out, lo_out, raw, hi_buf, lo_buf, load_sem, store_sem):
    def load(n):
        slot = n % DEPTH
        return pltpu.make_async_copy(leg.at[n], raw.at[slot], load_sem.at[slot])

    def store(n):
        slot = n % DEPTH
        return (
            pltpu.make_async_copy(hi_buf.at[slot], hi_out.at[n], store_sem.at[0, slot]),
            pltpu.make_async_copy(lo_buf.at[slot], lo_out.at[n], store_sem.at[1, slot]),
        )

    for n in range(DEPTH):
        load(n).start()

    def body(n, carry):
        load(n).wait()

        @pl.when(n >= DEPTH)
        def _():
            for copy in store(n - DEPTH):
                copy.wait()

        slot = n % DEPTH
        for t in range(2):
            hi, lo = split(raw[slot, pl.ds(t, ALL_ROWS, stride=2), :])
            hi_buf[slot, :, 128 * t : 128 * t + 128] = hi
            lo_buf[slot, :, 128 * t : 128 * t + 128] = lo
        for copy in store(n):
            copy.start()

        @pl.when(n + DEPTH < SLOTS)
        def _():
            load(n + DEPTH).start()

        return carry

    lax.fori_loop(0, SLOTS, body, 0)
    for n in range(SLOTS - DEPTH, SLOTS):
        for copy in store(n):
            copy.wait()


ANY = pl.BlockSpec(memory_space=pl.ANY)
ON_CHIP = pl.BlockSpec(memory_space=pltpu.VMEM)
SCALARS = pl.BlockSpec(memory_space=pltpu.SMEM)


def prepare(leg):
    shape = pltpu.HBM((SLOTS, ALL_ROWS, QLAT), BF16)
    buffer = pltpu.VMEM((DEPTH, ALL_ROWS, QLAT), BF16)
    return pl.pallas_call(
        prepare_kernel,
        in_specs=[ANY],
        out_specs=(ANY, ANY),
        out_shape=(shape, shape),
        scratch_shapes=[
            pltpu.VMEM((DEPTH, 2 * ALL_ROWS, 128), F32),
            buffer,
            buffer,
            pltpu.SemaphoreType.DMA((DEPTH,)),
            pltpu.SemaphoreType.DMA((2, DEPTH)),
        ],
        compiler_params=params(),
        cost_estimate=cost(11),
        name="prepare",
    )(in_hbm(leg))


def in_hbm(x):
    return pltpu.with_memory_space_constraint(x, pltpu.HBM)


RING = 12
AHEAD = 8
LEG_SCRATCH = [
    pltpu.VMEM((RING, ALL_ROWS, QLAT), BF16),
    pltpu.VMEM((RING, ALL_ROWS, QLAT), BF16),
    pltpu.SemaphoreType.DMA((2, RING)),
]


def slot_tables(n, hi_hbm, lo_hbm, leg_hi, leg_lo, sem):
    slot = n % RING
    return (
        pltpu.make_async_copy(hi_hbm.at[n], leg_hi.at[slot], sem.at[0, slot]),
        pltpu.make_async_copy(lo_hbm.at[n], leg_lo.at[slot], sem.at[1, slot]),
    )


def start_tables(count, *refs):
    for n in range(count):
        for copy in slot_tables(n, *refs):
            copy.start()


def next_tables(n, ahead, end, *refs):
    for copy in slot_tables(n, *refs):
        copy.wait()

    @pl.when(n + ahead < end)
    def _():
        for copy in slot_tables(n + ahead, *refs):
            copy.start()


def legendre_sums(pairs, place, own, right, left, far_a, far_b, leg_hi, leg_lo):
    return pl.pallas_call(
        legendre_kernel,
        in_specs=[SCALARS] * 2 + [ON_CHIP] * 5 + [ANY] * 2,
        out_specs=ON_CHIP,
        out_shape=jax.ShapeDtypeStruct((32, 8, 8, 128), F32),
        scratch_shapes=[pltpu.VMEM((1152, 128), F32), pltpu.VMEM((128, 1152), F32)] + LEG_SCRATCH,
        compiler_params=params(),
        cost_estimate=cost(10),
        name="legendre_sums",
    )(pairs, place, own, right, left, far_a, far_b, in_hbm(leg_hi), in_hbm(leg_lo))


def cos_sin(phase):
    quadrant = (phase + NLON // 8) >> 9
    x = (phase - (quadrant << 9)).astype(F32) * (2.0 * math.pi / NLON)
    y = x * x
    s = x * (1.0 + y * (-1 / 6 + y * (1 / 120 + y * (-1 / 5040 + y * (1 / 362880)))))
    c = 1.0 + y * (-1 / 2 + y * (1 / 24 + y * (-1 / 720 + y * (1 / 40320 + y * (-1 / 3628800)))))
    swap = (quadrant & 1) == 1
    cos = jnp.where(swap, s, c)
    sin = jnp.where(swap, c, s)
    cos = jnp.where(((quadrant + 1) & 2) != 0, -cos, cos)
    return cos, jnp.where((quadrant & 2) != 0, -sin, sin)


def table_kernel(orders, hi_out, lo_out, hi_buf, lo_buf, sem):
    def stores(n):
        rows = pl.ds(2 * n, 2)
        return (
            pltpu.make_async_copy(hi_buf.at[rows], hi_out.at[rows], sem.at[0, n]),
            pltpu.make_async_copy(lo_buf.at[rows], lo_out.at[rows], sem.at[1, n]),
        )

    def body(n, carry):
        table_pair(n, orders, hi_buf, lo_buf)
        for copy in stores(n):
            copy.start()
        return carry

    lax.fori_loop(0, 4, body, 0)
    for n in range(4):
        for copy in stores(n):
            copy.wait()


TABLE = pltpu.VMEM((8, QLAT, HALF), BF16)


def table_pair(n, orders, hi_ref, lo_ref):
    m = orders[n]
    product = m * lax.broadcasted_iota(jnp.int32, (1, 128), 1)
    cb, sb = cos_sin(product & (NLON - 1))
    factor = 1.0 / math.sqrt(NLON)
    cb, sb = cb * factor, sb * factor
    ca, sa = cos_sin((product & 15) << 7)
    for a in range(8):
        c1, s1 = ca[:, a : a + 1], sa[:, a : a + 1]
        for part, value in ((0, c1 * cb - s1 * sb), (1, -(s1 * cb + c1 * sb))):
            hi, lo = split(value)
            hi_ref[2 * n + part, :, 128 * a : 128 * a + 128] = hi
            lo_ref[2 * n + part, :, 128 * a : 128 * a + 128] = lo


def fourier_tables(pair_of_slot):
    first = pair_of_slot
    second = M - 1 - pair_of_slot
    flip = first % 2 == 1
    even = jnp.where(flip, second, first)
    odd = jnp.where(flip, first, second)
    orders = jnp.stack([even, odd], 0).reshape(2, QLAT, 2).transpose(0, 2, 1).reshape(4, QLAT, 1)
    orders = jnp.broadcast_to(orders, (4, QLAT, 128))
    shape = pltpu.HBM((8, QLAT, HALF), BF16)
    return pl.pallas_call(
        table_kernel,
        in_specs=[ON_CHIP],
        out_specs=(ANY, ANY),
        out_shape=(shape, shape),
        scratch_shapes=[TABLE, TABLE, pltpu.SemaphoreType.DMA((2, 4))],
        compiler_params=params(),
        cost_estimate=cost(5),
        name="tables",
    )(orders)


def table_loads(hi_hbm, lo_hbm, t_hi, t_lo, sem, nb):
    cols = pl.ds(256 * nb, 256)
    return (
        pltpu.make_async_copy(hi_hbm.at[:, :, cols], t_hi.at[:, :, cols], sem.at[0, nb]),
        pltpu.make_async_copy(lo_hbm.at[:, :, cols], t_lo.at[:, :, cols], sem.at[1, nb]),
    )


def to_grid(recv, hi_hbm, lo_hbm, t_hi, t_lo, sem, z):
    for nb in range(4):
        for copy in table_loads(hi_hbm, lo_hbm, t_hi, t_lo, sem, nb):
            copy.start()
    for j in range(8):
        hi, lo = split(recv[:, j, :].T)
        for n in range(8):
            z[n, 16 * j : 16 * j + 16, :] = hi[16 * n : 16 * n + 16]
            z[n, 128 + 16 * j : 128 + 16 * j + 16, :] = lo[16 * n : 16 * n + 16]

    def block(nb):
        cols = slice(256 * nb, 256 * nb + 256)
        for copy in table_loads(hi_hbm, lo_hbm, t_hi, t_lo, sem, nb):
            copy.wait()
        res = []
        for par in range(2):
            wide = jnp.zeros((256, 256), F32)
            narrow = jnp.zeros((128, 256), F32)
            for s in range(2):
                for p in range(2):
                    lhs = z[s * 4 + par * 2 + p]
                    n = par * 4 + s * 2 + p
                    wide = wide + mm(lhs, t_hi[n, :, cols])
                    narrow = narrow + mm(lhs[0:128], t_lo[n, :, cols])
            res.append(wide[0:128] + wide[128:256] + narrow)
        return res[0] + res[1], res[0] - res[1]

    return block


def fold(west, east, d, nb):
    cols = slice(256 * nb, 256 * nb + 256)
    for par, value in ((0, west + east), (1, west - east)):
        hi, lo = split(value)
        d[par, 0:128, cols] = hi
        d[par, 128:256, cols] = lo


def from_grid(d, t_hi, t_lo, res, out):
    for par in range(2):
        for s in range(2):
            for p in range(2):
                n = par * 4 + s * 2 + p
                wide = mm_t(d[par], t_hi[n])
                narrow = mm_t(d[par, 0:128], t_lo[n])
                res[s * 4 + par * 2 + p] = wide[0:128] + wide[128:256] + narrow
    for j in range(8):
        rows = jnp.concatenate([res[n, 16 * j : 16 * j + 16, :] for n in range(8)], axis=0)
        out[:, j, :] = rows.T


def wind_kernel(
    recv, hi_hbm, lo_hbm, out, wind, last, first, speed_ref, z, d, res, t_hi, t_lo, sem, g
):
    block = to_grid(recv, hi_hbm, lo_hbm, t_hi, t_lo, sem, z)
    for nb in range(4):
        tend = []
        for side, value in enumerate(block(nb)):
            cols = slice(HALF * side + 256 * nb, HALF * side + 256 * nb + 256)
            for t in range(2):
                g[8 * side + 2 * nb + t] = value[:, 128 * t : 128 * t + 128]
            both = value.reshape(8, 16, 256)
            u, v = both[:, 0:8], both[:, 8:16]
            speed = jnp.sqrt(u * u + v * v + 1.0)
            speed_ref[:, cols] = speed.reshape(64, 256)
            drag = -DRAG_COEFFICIENT * speed
            tend.append(jnp.concatenate([drag * u, drag * v], axis=1).reshape(128, 256))
        fold(tend[0], tend[1], d, nb)
    for t in range(16):
        for l in range(TLEV):
            cols = slice(128 * t, 128 * t + 128)
            for n, value in (
                (l, g[t, pl.ds(l, 8, stride=16), :]),
                (TLEV + l, -g[t, pl.ds(8 + l, 8, stride=16), :]),
            ):
                wind[n, :, cols] = value
                last[n, :, cols] = value[4:8]
                first[n, :, cols] = value[0:4]
    from_grid(d, t_hi, t_lo, res, out)


def moist_kernel(
    recv, hi_hbm, lo_hbm, speed_ref, heat_ref, out, z, d, res, t_hi, t_lo, sem
):
    block = to_grid(recv, hi_hbm, lo_hbm, t_hi, t_lo, sem, z)
    for nb in range(4):
        tend = []
        for side, value in enumerate(block(nb)):
            cols = slice(HALF * side + 256 * nb, HALF * side + 256 * nb + 256)
            both = value.reshape(8, 16, 256)
            t, q = both[:, 0:8], both[:, 8:16]
            speed = speed_ref[:, cols].reshape(8, 8, 256)
            n = 8 * side + 2 * nb
            heat = jnp.concatenate([heat_ref[n], heat_ref[n + 1]], axis=1).reshape(8, 8, 256)
            source = MOISTURE_SOURCE * t * q
            tend.append(
                jnp.concatenate(
                    [heat - source, source - RAINFALL_FACTOR * speed * q], axis=1
                ).reshape(128, 256)
            )
        fold(tend[0], tend[1], d, nb)
    from_grid(d, t_hi, t_lo, res, out)


FOURIER_SCRATCH = [
    pltpu.VMEM((8, 256, 256), BF16),
    pltpu.VMEM((2, 256, HALF), BF16),
    pltpu.VMEM((8, 128, 256), F32),
    TABLE,
    TABLE,
    pltpu.SemaphoreType.DMA((2, 4)),
]


def wind_stage(recv, t_hi, t_lo):
    return pl.pallas_call(
        wind_kernel,
        in_specs=[ON_CHIP, ANY, ANY],
        out_shape=(
            jax.ShapeDtypeStruct((QLAT, 8, 128), F32),
            jax.ShapeDtypeStruct((2 * TLEV, 8, NLON), F32),
            jax.ShapeDtypeStruct((2 * TLEV, 4, NLON), F32),
            jax.ShapeDtypeStruct((2 * TLEV, 4, NLON), F32),
            jax.ShapeDtypeStruct((64, NLON), F32),
        ),
        scratch_shapes=FOURIER_SCRATCH + [pltpu.VMEM((16, 128, 128), F32)],
        compiler_params=params(),
        cost_estimate=cost(10),
        name="wind_stage",
    )(recv, in_hbm(t_hi), in_hbm(t_lo))


def moist_stage(recv, t_hi, t_lo, speed, heat):
    return pl.pallas_call(
        moist_kernel,
        in_specs=[ON_CHIP, ANY, ANY, ON_CHIP, ON_CHIP],
        out_shape=jax.ShapeDtypeStruct((QLAT, 8, 128), F32),
        scratch_shapes=FOURIER_SCRATCH,
        compiler_params=params(),
        cost_estimate=cost(10),
        name="moist_stage",
    )(recv, in_hbm(t_hi), in_hbm(t_lo), speed, heat)


def halo_of(above, below):
    return jnp.concatenate([below, above], axis=0)


def vertical(middle, halo, row):
    up_m, up_h = pltpu.roll(middle, 7, 0), pltpu.roll(halo, 7, 0)
    down_m, down_h = pltpu.roll(middle, 1, 0), pltpu.roll(halo, 1, 0)
    end, start = row == 7, row == 0
    return (
        (jnp.where(end, up_h, up_m), jnp.where(start, down_h, down_m)),
        (jnp.where(end, up_m, up_h), jnp.where(start, down_m, down_h)),
    )


def advect_kernel(
    rate, band, tracer, above, below, wind, wind_above, wind_below, out, heat, coef, total
):
    k = pl.program_id(0)
    row = lax.broadcasted_iota(jnp.int32, (8, 1), 0)

    @pl.when(k == 0)
    def _():
        for l in range(TLEV):
            m = TLEV + l
            u = (wind[l], halo_of(wind_above[l], wind_below[l]))
            w = (wind[m], halo_of(wind_above[m], wind_below[m]))
            moved = vertical(*w, row)
            faces = []
            for n, offset in ((0, row), (1, jnp.where(row < 4, row + 8, row - 8))):
                upper = band[0] * 8 + offset
                inside = (upper >= 0) & (upper <= NLAT - 2)
                faces.append(jnp.where(inside, 0.5 * (w[n] + moved[n][0]), 0.0))
            above_faces = vertical(*faces, row)
            for n in range(2):
                east = 0.5 * (u[n] + pltpu.roll(u[n], NLON - 1, 1))
                west = pltpu.roll(east, 1, 1)
                south, north = faces[n], above_faces[n][1]
                here = (
                    jnp.maximum(east, 0.0) - jnp.minimum(west, 0.0)
                    + jnp.maximum(south, 0.0) - jnp.minimum(north, 0.0)
                )
                stencil = (
                    -COURANT * here,
                    -COURANT * jnp.minimum(east, 0.0),
                    COURANT * jnp.maximum(west, 0.0),
                    -COURANT * jnp.minimum(south, 0.0),
                    COURANT * jnp.maximum(north, 0.0),
                )
                for c, value in enumerate(stencil):
                    coef[l, n, c] = value
        total[...] = jnp.zeros(total.shape, F32)

    def advect(field, l, parts):
        moved = vertical(*field, row)
        done = []
        for n in range(parts):
            q = field[n]
            south, north = moved[n]
            done.append(
                coef[l, n, 0] * q
                + coef[l, n, 1] * pltpu.roll(q, NLON - 1, 1)
                + coef[l, n, 2] * pltpu.roll(q, 1, 1)
                + coef[l, n, 3] * south
                + coef[l, n, 4] * north
            )
        return done

    for l in range(TLEV):
        q = (tracer[0, l], halo_of(above[0, l], below[0, l]))
        first = [a + b for a, b in zip(q, advect(q, l, 2))]
        second = [
            0.75 * a + 0.25 * (b + c) for a, b, c in zip(q, first, advect(first, l, 2))
        ]
        new = q[0] / 3.0 + 2.0 / 3.0 * (second[0] + advect(second, l, 1)[0])
        out[0, l] = new
        total[l] = total[l] + rate[k, l] * new

    @pl.when(k == NTR - 1)
    def _():
        heat[...] = jnp.zeros(heat.shape, F32)
        for t in range(16):
            for l in range(TLEV):
                heat[t, pl.ds(l, 8, stride=8), :] = total[l, :, 128 * t : 128 * t + 128]


def transport(rate, band, tracers, above, below, wind, wind_above, wind_below):
    block = pl.BlockSpec((1, TLEV, 8, NLON), lambda k, *_: (k, 0, 0, 0))
    edge = pl.BlockSpec((1, TLEV, 4, NLON), lambda k, *_: (k, 0, 0, 0))
    whole = pl.BlockSpec((2 * TLEV, 8, NLON), lambda k, *_: (0, 0, 0))
    side = pl.BlockSpec((2 * TLEV, 4, NLON), lambda k, *_: (0, 0, 0))
    return pl.pallas_call(
        advect_kernel,
        grid_spec=pltpu.PrefetchScalarGridSpec(
            num_scalar_prefetch=2,
            grid=(NTR,),
            in_specs=[block, edge, edge, whole, side, side],
            out_specs=(block, pl.BlockSpec((16, 64, 128), lambda k, *_: (0, 0, 0))),
            scratch_shapes=[
                pltpu.VMEM((TLEV, 2, 5, 8, NLON), F32),
                pltpu.VMEM((TLEV, 8, NLON), F32),
            ],
        ),
        out_shape=(
            jax.ShapeDtypeStruct((NTR, TLEV, 8, NLON), F32),
            jax.ShapeDtypeStruct((16, 64, 128), F32),
        ),
        compiler_params=params(dimension_semantics=("arbitrary",)),
        cost_estimate=cost(10),
        name="transport",
    )(rate, band, tracers, above, below, wind, wind_above, wind_below)


PART_ROWS = ALL_ROWS // 2


def tendency_kernel(
    half, pairs, place, recv, weight, hi_hbm, lo_hbm,
    own, ahead, far, behind, res, leg_hi, leg_lo, sem,
):
    slots = pl.ds(half * (SLOTS // 2), SLOTS // 2)
    tables = (hi_hbm.at[slots], lo_hbm.at[slots], leg_hi, leg_lo, sem)
    start_tables(4, *tables)

    def body(step, carry):
        tendency_group(
            half, step, pairs, place, recv, weight, tables, own, ahead, far, behind, res
        )
        return carry

    lax.fori_loop(0, 2, body, 0)


def tendency_group(
    half, step, pairs, place, recv, weight, tables, own, ahead, far, behind, res
):
    _, _, leg_hi, leg_lo, _ = tables
    d = place[0]
    lane = lax.broadcasted_iota(jnp.int32, (1, 128), 1)
    rhs = []
    bound = jnp.zeros((1, 128), jnp.int32)
    for b in range(4):
        lo_order = pairs[8 * half + 4 * step + b]
        f = recv[:, 4 * half + 2 * step + b // 2].reshape(QLAT, 128) * weight[...]
        even = pltpu.roll(f, (32 * b - 64 * (b % 2)) % 128, 1)
        odd = pltpu.roll(f, (32 * b - 64 * (b % 2) - 32) % 128, 1)
        here = lane // 32 == b
        flip = lo_order % 2 == 1
        low = jnp.where(here, jnp.where(flip, odd, even), 0.0)
        high = jnp.where(here, jnp.where(flip, even, odd), 0.0)
        rhs.append(split(jnp.concatenate([low, high], axis=1)))
        bound = jnp.where(here, M - lo_order, bound)
    rhs = jnp.concatenate([x for hi, lo in rhs for x in (hi, lo, hi)], axis=0)
    for b in range(4):
        next_tables(4 * step + b, 4, SLOTS // 2, *tables)
    for part in range(2):
        rows = slice(PART_ROWS * part, PART_ROWS * (part + 1))
        lhs = []
        for b in range(4):
            n = (4 * step + b) % RING
            hi = leg_hi[n, rows, :]
            lhs += [hi, hi, leg_lo[n, rows, :]]
        both = mm(jnp.concatenate(lhs, axis=1), rhs)
        r = PART_ROWS * part + lax.broadcasted_iota(jnp.int32, (PART_ROWS, 1), 0)
        value = jnp.where(r < bound, both[:, 0:128], both[:, 128:256])
        res[rows, :] = jnp.where(r <= M, value, 0.0)

    def get(k):
        return res[pl.ds(pl.multiple_of(((d + k) % 4) * ROWS, 8), ROWS), :]

    own[step] = get(0)
    ahead[step] = get(1)
    far[step] = get(2)
    behind[step] = get(3)


def tendency_sums(half, pairs, place, recv, weight, leg_hi, leg_lo):
    part = jax.ShapeDtypeStruct((2, ROWS, 128), F32)
    return pl.pallas_call(
        functools.partial(tendency_kernel, half),
        in_specs=[SCALARS] * 2 + [ON_CHIP] * 2 + [ANY] * 2,
        out_specs=(ON_CHIP,) * 4,
        out_shape=(part,) * 4,
        scratch_shapes=[pltpu.VMEM((ALL_ROWS, 128), F32)] + LEG_SCRATCH,
        compiler_params=params(),
        cost_estimate=cost(6),
        name="tendency_sums",
    )(pairs, place, recv, weight, in_hbm(leg_hi), in_hbm(leg_lo))


def unpack_kernel(*refs):
    *pieces, out, scr = refs
    for ch in range(2):
        for g in range(4):
            first = 6 * ch + 3 * (g // 2)
            own, ahead, behind = pieces[first : first + 3]
            scr[0:ROWS, :] = own[g % 2] + ahead[g % 2] + behind[g % 2]
            value = scr[...].T
            for s in range(4):
                for p in range(2):
                    r0 = s * 32 + p * 16
                    c0 = p * 32 + ch * 16
                    out[4 * g + s, c0 : c0 + 16, :] = value[r0 : r0 + 16, 0:ROWS]


def unpack(pieces):
    return pl.pallas_call(
        unpack_kernel,
        out_shape=jax.ShapeDtypeStruct((SLOTS, 64, ROWS), F32),
        scratch_shapes=[pltpu.VMEM((384, 128), F32)],
        compiler_params=params(),
        cost_estimate=cost(4),
        name="unpack",
    )(*pieces)


def shift(x, axis, by):
    n = lax.axis_size(axis)
    return lax.ppermute(x, axis, [(i, (i + by) % n) for i in range(n)])


def neighbours(last, first):
    axes = ("ma", "pb")
    n = lax.axis_size("ma") * lax.axis_size("pb")
    down = [(i, i + 1) for i in range(n - 1)]
    return (
        lax.ppermute(last, axes, down),
        lax.ppermute(first, axes, [(b, a) for a, b in down]),
    )


def gather_rows(x):
    right = shift(x, "pb", 1)
    left = shift(x, "pb", -1)
    return right, left, shift(right[0:2], "pb", 1), shift(left[2:4], "pb", -1)


def scatter_rows(recv, *args):
    own_0, ahead_0, far_0, behind_0 = tendency_sums(0, *args[:2], recv, *args[2:])
    via_0 = shift(far_0, "pb", 1)
    behind_0 = shift(behind_0, "pb", -1)
    own_1, ahead_1, far_1, behind_1 = tendency_sums(1, *args[:2], recv, *args[2:])
    via_1 = shift(far_1, "pb", -1)
    ahead_1 = shift(ahead_1, "pb", 1)
    ahead_0 = ahead_0 + via_0
    ahead_0 = shift(ahead_0, "pb", 1)
    behind_1 = behind_1 + via_1
    behind_1 = shift(behind_1, "pb", -1)
    return own_0, ahead_0, behind_0, own_1, ahead_1, behind_1


def exchange(x):
    return lax.all_to_all(x, "ma", 0, 0, tiled=True)


def shards(coefs, legendre, quad_weight, pair_of_slot, tracers, heat_rate):
    ma = lax.axis_index("ma")
    pb = lax.axis_index("pb")
    pairs = lax.dynamic_slice_in_dim(pair_of_slot, ma * SLOTS, SLOTS, 0)
    place = pb.reshape(1).astype(jnp.int32)
    band = (ma * lax.axis_size("pb") + pb).reshape(1).astype(jnp.int32)
    leg = legendre.reshape(SLOTS, 2 * ALL_ROWS, 128)
    weight = jnp.broadcast_to(quad_weight.reshape(QLAT, 1), (QLAT, 128))

    rows_a, rows_b = pack(jnp.transpose(coefs, (0, 2, 1)))
    got_a = gather_rows(rows_a)
    rows_b, near_a = lax.optimization_barrier((rows_b, got_a[0:2]))
    got_a = (*near_a, *got_a[2:])
    got_b = gather_rows(rows_b)
    t_hi, t_lo = fourier_tables(pair_of_slot)
    leg_hi, leg_lo = prepare(leg)
    sums_a = legendre_sums(pairs, place, rows_a, *got_a, leg_hi, leg_lo)
    sent_a = exchange(sums_a)
    above, below = neighbours(tracers[:, :, 4:8, :], tracers[:, :, 0:4, :])
    sums_b = legendre_sums(pairs, place, rows_b, *got_b, leg_hi, leg_lo)
    sent_b = exchange(sums_b)

    back_a, wind, last, first, speed = wind_stage(sent_a.reshape(QLAT, 8, 128), t_hi, t_lo)
    wind_above, wind_below = neighbours(last, first)
    back_a = exchange(back_a.reshape(32, 8, 8, 128))
    new_tracers, heat = transport(
        heat_rate, band, tracers, above, below, wind, wind_above, wind_below
    )
    back_b = moist_stage(sent_b.reshape(QLAT, 8, 128), t_hi, t_lo, speed, heat)
    back_b = exchange(back_b.reshape(32, 8, 8, 128))
    sums_a = scatter_rows(back_a, pairs, place, weight, leg_hi, leg_lo)
    sums_b = scatter_rows(back_b, pairs, place, weight, leg_hi, leg_lo)
    summed = unpack((*sums_a, *sums_b))
    return (jnp.transpose(summed, (0, 2, 1)), new_tracers)


def solution(mesh):
    in_specs = (
        P("ma", "pb", None),
        P("ma", None, "pb", None),
        P("pb", None),
        P(),
        P(None, None, ("ma", "pb"), None),
        P(),
    )
    out_specs = (P("ma", "pb", None), P(None, None, ("ma", "pb"), None))
    return jax.shard_map(shards, mesh=mesh, in_specs=in_specs, out_specs=out_specs, check_vma=False)
```
